32 devices in a mesh: enc: 8 (over z, x), section: 2 (over core), llmdp: 2 (over y).
Axes of the slice: x: 2, y: 2, z: 4, core: 2. Of those that a mesh axis runs over, the one named last changes fastest.
Arguments:
- patches: bfloat16 [2048, 3200], P('enc', ('section', 'llmdp')), may hold values from -6 to 6
- gain: float32 [3200], replicated, may hold values from 0.25 to 1.75
- shift: float32 [3200], replicated, may hold values from -3 to 3
- proj_weight: bfloat16 [3200, 8192], P('enc', ('section', 'llmdp')), may hold values from -0.109375 to 0.109375
- llm_rank: int32 [2048, 1], P('enc'), may hold values from 0 to 7; in each aligned block of 256 rows (0 to 255, 256 to 511, ...) at most 96 rows name the same one
- embed_grad: bfloat16 [6144, 8192], P('enc', ('section', 'llmdp')), may hold values from -0.59765625 to 0.59765625
Outputs:
- embeds_recv: bfloat16 [6144, 8192], P('enc', ('section', 'llmdp'))
- hidden_state_gradient: bfloat16 [2048, 3200], P('enc', ('section', 'llmdp'))
- grad_weight: float32 [3200, 8192], P('enc', ('section', 'llmdp'))
- gain_gradient: float32 [3200], P(('section', 'llmdp'))
- grad_shift: float32 [3200], P(('section', 'llmdp'))
The draws below stay inside these ranges and needn't reach their ends.
Inputs may be any that keep to these rules, and one draw needn't show every extreme that they name: `llm_rank`: among the 256 rows of one device, at most 96 name the same owner, a bound that some block reaches.
All inputs are finite; a program needn't handle non-finite values.
Results may differ from the reference program's by a relative error of at most 0.018.
Values may be sent and summed in bfloat16 or wider, within the bound.
A program may use at most 128 MiB of HBM per device.

```python
import math
import jax
import jax.numpy as jnp
import numpy as np
from jax import lax

D = 3200
E = 8192
TOK_DEV = 256
TOKENS = 2048
MOST = 96
RECV = 6144
N_ENC = 8
N_SECTION = 2
N_LLMDP = 2


def level_of(own_key, shape, split, least, largest):
    factor_of = 1.0
    for axis_at, blocks in split:
        steps = jax.random.uniform(jax.random.fold_in(jax.random.fold_in(own_key, 6), axis_at), (blocks,), jnp.float32, least / len(split), largest / len(split))
        factor_of = factor_of * jnp.repeat(jnp.exp(steps), shape[axis_at] // blocks).reshape((-1,) + (1,) * (len(shape) - 1 - axis_at))
    return factor_of


def shared_out(stream_key, own, number, rows, count, top, limit, lean):
    order = jax.random.permutation(stream_key, count)
    heavy_load, common = portions_of(count, rows * top, limit, lean, True), portions_of(count, rows * top, limit, lean, False)
    places = jnp.arange(count)

    def named(sizes, turn):
        used = int((sizes > 0).sum())
        fixed = max(1, used // 4)
        moved = fixed + (places - fixed + turn * (used - fixed)) % max(1, count - fixed)
        return jnp.zeros((count,), jnp.int32).at[order[jnp.where(places < fixed, places, moved)]].set(jnp.asarray(sizes, jnp.int32))

    sizes = jnp.where(number % 4 == 0, named(heavy_load, number // 4), named(common, number - number // 4 - 1))
    mixed = jax.random.permutation(jax.random.fold_in(own, 3), count)
    source_of, receiver = mixed[0:count // 2 * 2:2], mixed[1:count // 2 * 2:2]
    slack = jnp.minimum(sizes[source_of] - 1, limit - sizes[receiver]) // 2
    slack = jnp.where((source_of == order[0]) | (receiver == order[0]) | (sizes[receiver] == 0), 0, jnp.maximum(slack, 0))
    moved = jax.random.randint(jax.random.fold_in(own, 4), (count // 2,), 0, 1 << 20) % (slack + 1)
    sizes = sizes.at[source_of].add(-moved).at[receiver].add(moved)
    labels = jnp.searchsorted(jnp.cumsum(sizes), jnp.arange(rows * top), side="right").astype(jnp.int32)
    listing = labels.reshape(top, rows).T
    listing = listing[jax.random.permutation(jax.random.fold_in(own, 1), rows)]
    turn = jax.random.randint(jax.random.fold_in(own, 2), (rows, 1), 0, top)
    return jnp.take_along_axis(listing, (jnp.arange(top)[None, :] + turn) % top, axis=1)


def portions_of(count, total, reach, slope, full):
    weights = [(1 << 20) // math.isqrt(grade ** slope) + 1 for grade in range(1, count + 1)]
    largest = reach if full else min(reach, max(-(-total // count), total * weights[0] // sum(weights)))
    least = 1 if total - largest >= count - 1 else 0
    counts, spare = [largest] + [least] * (count - 1), total - largest - least * (count - 1)
    while spare > 0:
        movable = [i for i in range(1, count) if counts[i] < largest] or [i for i in range(1, count) if counts[i] < reach]
        whole, remaining = sum([weights[i] for i in movable]), spare
        for i in movable:
            more = min(reach - counts[i], max(1, remaining * weights[i] // whole), spare)
            counts[i] = counts[i] + more
            spare = spare - more
    return np.array(counts)


def noise(own_key, extent, scale, most, pieces=(), held_as=jnp.bfloat16):
    factor_of = level_of(own_key, extent, pieces, -0.22, 0.18) if pieces else 1.0
    array = jax.random.normal(own_key, extent, jnp.float32) * scale * factor_of
    return jnp.minimum(jnp.maximum(array, -most), most).astype(held_as)


def setup_inputs(seed: int = 0) -> dict:
    arg_keys = jax.random.split(jax.random.key(seed), 7)
    patches = noise(arg_keys[0], (TOKENS, D), 1.0, 6.0, ((0, 8), (1, 4)))
    gain = jnp.clip(1.0 + 0.15 * jax.random.normal(arg_keys[1], (D,), jnp.float32), 0.25, 1.75)
    shift = noise(arg_keys[2], (D,), 0.5, 3.0, (), jnp.float32)
    proj_weight = noise(arg_keys[3], (D, E), D ** -0.5, 0.109375, ((0, 8), (1, 4)))
    llm_rank_keys = jax.random.split(jax.random.fold_in(arg_keys[4], 1), TOKENS // TOK_DEV)
    llm_rank_turns = jax.random.permutation(jax.random.fold_in(arg_keys[4], 3), TOKENS // TOK_DEV)
    llm_rank = jax.vmap(lambda own, number: shared_out(jax.random.fold_in(arg_keys[4], 2), own, number, TOK_DEV, N_ENC, 1, MOST, 2))(llm_rank_keys, llm_rank_turns).reshape((TOKENS, 1))
    embed_grad = noise(arg_keys[5], (RECV, E), 0.1, 0.59765625, ((0, 8), (1, 4)))
    return {"patches": patches, "gain": gain, "shift": shift, "proj_weight": proj_weight, "llm_rank": llm_rank, "embed_grad": embed_grad}


EPSILON = 1e-05

def reference(patches, gain, shift, proj_weight, llm_rank, embed_grad):
    value_entries = patches.astype(jnp.float32)
    row_average = lax.optimization_barrier(jnp.mean(value_entries, 1, keepdims=True))
    variance = lax.optimization_barrier(jnp.mean(value_entries * value_entries, 1, keepdims=True)) - row_average * row_average
    inverse_deviation = lax.rsqrt(variance + EPSILON)
    standardized_rows = (value_entries - row_average) * inverse_deviation
    normed_hidden = (standardized_rows * gain + shift).astype(jnp.bfloat16)
    embed = jnp.dot(normed_hidden, proj_weight, preferred_element_type=jnp.float32).astype(jnp.bfloat16)
    target = llm_rank[:, 0].astype(jnp.int32).reshape(N_ENC, TOK_DEV)
    owners = jnp.arange(N_ENC, dtype=jnp.int32)
    hits = (target[:, :, None] == owners[None, None, :]).astype(jnp.int32)
    rank = lax.optimization_barrier(jnp.sum((jnp.cumsum(hits, 1) - hits) * hits, 2)).astype(jnp.int32)
    slot = (target * (N_ENC * MOST) + owners[:, None] * MOST + rank).reshape(-1).astype(jnp.int32)
    embeds_recv = jnp.zeros((RECV, E), jnp.bfloat16).at[slot].set(embed)
    d_embed = embed_grad[slot]
    groups = N_SECTION * N_LLMDP
    group_cols = E // groups

    def group_step(total, index):
        start = (index * group_cols).astype(jnp.int32)
        grad_part = lax.dynamic_slice_in_dim(d_embed, start, group_cols, 1)
        weight_part = lax.dynamic_slice_in_dim(proj_weight, start, group_cols, 1)
        term = lax.dot_general(grad_part, weight_part, (((1,), (1,)), ((), ())), preferred_element_type=jnp.float32)
        return (total + lax.optimization_barrier(term.astype(jnp.bfloat16)).astype(jnp.float32), None)
    normalized_gradient, _ = lax.scan(group_step, jnp.zeros((TOKENS, D), jnp.float32), jnp.arange(groups, dtype=jnp.int32))

    def block_step(total, pair):
        term = lax.dot_general(pair[0], pair[1], (((0,), (0,)), ((), ())), preferred_element_type=jnp.float32)
        return (total + lax.optimization_barrier(term.astype(jnp.bfloat16)).astype(jnp.float32), None)
    grad_weight, _ = lax.scan(block_step, jnp.zeros((D, E), jnp.float32), (normed_hidden.reshape(N_ENC, TOK_DEV, D), d_embed.reshape(N_ENC, TOK_DEV, E)))
    centered_gradient = normalized_gradient * gain
    gradient_row_average = lax.optimization_barrier(jnp.mean(centered_gradient, 1, keepdims=True))
    gradient_cross_product = lax.optimization_barrier(jnp.mean(centered_gradient * standardized_rows, 1, keepdims=True))
    hidden_state_gradient = (inverse_deviation * (centered_gradient - gradient_row_average - standardized_rows * gradient_cross_product)).astype(jnp.bfloat16)
    gain_gradient = lax.optimization_barrier(jnp.sum(normalized_gradient * standardized_rows, 0))
    grad_shift = lax.optimization_barrier(jnp.sum(normalized_gradient, 0))
    return (embeds_recv, hidden_state_gradient, grad_weight, gain_gradient, grad_shift)
```

```python
import functools

import jax
import jax.numpy as jnp
from jax import lax
from jax.experimental import pallas as pl
from jax.experimental.pallas import tpu as pltpu
from jax.sharding import PartitionSpec as P

EPSILON = 1e-05
MESH = pl.DeviceIdType.MESH
F32 = jnp.float32
BF16 = jnp.bfloat16

MAX_BLOCK = 2
SUBLANES = 16
LANES = 128


def block_size(senders, out_cols):
    size = MAX_BLOCK
    while size > 1 and (senders % size or senders == size or out_cols % (size * 128)):
        size //= 2
    return size


def slots_of(llm_rank, senders, most_slots):
    target = llm_rank[:, 0]
    owners = jnp.arange(senders, dtype=jnp.int32)
    hits = (target[:, None] == owners[None, :]).astype(jnp.int32)
    rank = jnp.sum((jnp.cumsum(hits, 0) - hits) * hits, 1)
    return target * most_slots + rank


class Place:
    def __init__(self):
        self.e = lax.axis_index("enc")
        self.k = lax.axis_index("section")
        self.y = lax.axis_index("llmdp")
        self.x = lax.rem(self.e, 2)
        self.senders = lax.axis_size("enc")
        self.c = self.group(self.k, self.y)
        self.x_peer = (self.e + 1 - 2 * self.x, self.k, self.y)
        self.y_peer = (self.e, self.k, 1 - self.y)
        self.k_peer = (self.e, 1 - self.k, self.y)

    def group(self, k, y):
        return k * 2 + y

    def other(self, step):
        return lax.rem(self.e + step, self.senders)

    def greet(self):
        barrier = pltpu.get_barrier_semaphore()

        def one(step, carry):
            pl.semaphore_signal(
                barrier, inc=1, device_id=(self.other(step), self.k, self.y), device_id_type=MESH
            )
            return carry

        lax.fori_loop(1, self.senders, one, 0)
        for peer in (self.y_peer, self.k_peer):
            pl.semaphore_signal(barrier, inc=1, device_id=peer, device_id_type=MESH)
        pl.semaphore_wait(barrier, self.senders + 1)


def send(src, dst, send_sem, recv_sem, device):
    return pltpu.make_async_remote_copy(
        src_ref=src, dst_ref=dst, send_sem=send_sem, recv_sem=recv_sem, device_id=device, device_id_type=MESH
    )


def spread_kernel(
    out_ref, eg_ref, gw_ref, n_ref, eg_out,
    nv, eg_v, route_s, route_r, x_s, x_r, y_s, y_r, d_s, d_r, eg_sem, local_sem, n_sem,
):
    at = Place()
    senders, most, width = out_ref.shape
    half = eg_v.shape[2]
    rows = eg_v.shape[1]
    e, k, y, x, c = at.e, at.k, at.y, at.x, at.c
    ox = 1 - x
    c_y, c_k, c_ky = at.group(k, 1 - y), at.group(1 - k, y), at.group(1 - k, 1 - y)

    def route(d):
        return send(out_ref.at[d], nv.at[c, lax.rem(d, 2), e], route_s.at[d], route_r.at[e], (d, k, y))

    def route_in(s):
        return send(out_ref.at[s], nv.at[c, x, s], route_s.at[s], route_r.at[s], (s, k, y))

    def x_hop(s, src):
        return send(src, nv.at[c, x, s], x_s.at[s], x_r.at[s], at.x_peer)

    def x_in(s):
        return send(nv.at[c, ox, s], nv.at[c, ox, s], x_s.at[s], x_r.at[s], at.x_peer)

    def y_hop(w, s, src):
        return send(src, nv.at[c, w, s], y_s.at[w, s], y_r.at[w, s], at.y_peer)

    def y_in(w, s):
        return send(nv.at[c_y, w, s], nv.at[c_y, w, s], y_s.at[w, s], y_r.at[w, s], at.y_peer)

    def k_hop(v, w, s, src):
        return send(src, nv.at[at.group(k, v), w, s], d_s.at[v, w, s], d_r.at[v, w, s], at.k_peer)

    def k_in(v, w, s):
        ref = nv.at[at.group(1 - k, v), w, s]
        return send(ref, ref, d_s.at[v, w, s], d_r.at[v, w, s], at.k_peer)

    eg_send = send(
        eg_ref.at[:, pl.ds(pl.multiple_of(ox * half, LANES), half)], eg_v.at[x], eg_sem.at[0], eg_sem.at[1], at.x_peer
    )
    eg_load = pltpu.make_async_copy(
        eg_ref.at[:, pl.ds(pl.multiple_of(x * half, LANES), half)], eg_v.at[x], local_sem.at[0]
    )
    eg_in = send(eg_v.at[ox], eg_v.at[ox], eg_sem.at[0], eg_sem.at[1], at.x_peer)

    eg_load.start()
    at.greet()

    def over(fn, start=0):
        lax.fori_loop(start, senders, lambda i, carry: (fn(i), carry)[1], 0)

    over(lambda step: route(at.other(step)).start(), 1)
    own = out_ref.at[e]
    x_hop(e, own).start()
    y_hop(x, e, own).start()
    k_hop(y, x, e, own).start()
    nv[c, x, e] = out_ref[e]

    def pass_on(step):
        s = at.other(step)
        ref = nv.at[c, x, s]
        route_in(s).wait_recv()
        x_hop(s, ref).start()
        y_hop(x, s, ref).start()
        k_hop(y, x, s, ref).start()

    over(pass_on, 1)
    eg_send.start()

    def pass_x(step):
        s = at.other(step)
        ref = nv.at[c, ox, s]
        x_in(s).wait_recv()
        y_hop(ox, s, ref).start()
        k_hop(y, ox, s, ref).start()

    over(pass_x)

    def product(group):
        total = None
        for w in range(2):
            term = lax.dot_general(
                nv[group, w].reshape(rows, width), eg_v[w], (((0,), (0,)), ((), ())), preferred_element_type=F32
            )
            total = term if total is None else total + term
        gw_ref[pl.ds(pl.multiple_of(group * width, SUBLANES), width), :] = total.astype(BF16)

    def keep(i, group):
        pltpu.make_async_copy(nv.at[group], n_ref.at[group], n_sem.at[i]).start()

    def pass_y(w):
        def one(step):
            s = at.other(step)
            y_in(w, s).wait_recv()
            k_hop(1 - y, w, s, nv.at[c_y, w, s]).start()

        over(one)

    keep(0, c)
    eg_load.wait()
    eg_in.wait_recv()
    eg_keep = pltpu.make_async_copy(eg_v, eg_out, local_sem.at[0])
    eg_keep.start()
    product(c)
    pass_y(x)

    def near_in(step):
        for w in range(2):
            k_in(y, w, at.other(step)).wait_recv()

    over(near_in)
    keep(1, c_k)
    product(c_k)
    pass_y(ox)
    keep(2, c_y)
    product(c_y)

    def far_in(step):
        for w in range(2):
            k_in(1 - y, w, at.other(step)).wait_recv()

    over(far_in)
    keep(3, c_ky)
    product(c_ky)

    over(lambda step: route(at.other(step)).wait_send(), 1)

    def sent(step):
        s = at.other(step)
        x_hop(s, nv.at[c, x, s]).wait_send()
        for w in range(2):
            y_hop(w, s, nv.at[c, w, s]).wait_send()
            for v in range(2):
                k_hop(v, w, s, nv.at[at.group(k, v), w, s]).wait_send()

    over(sent)
    eg_send.wait_send()
    eg_keep.wait()
    for i, group in enumerate((c, c_k, c_y, c_ky)):
        pltpu.make_async_copy(nv.at[group], n_ref.at[group], n_sem.at[i]).wait()


def spread(outgoing, embed_grad):
    senders, most, width = outgoing.shape
    groups = 4
    rows, cols = embed_grad.shape
    half = cols // 2
    dma = pltpu.SemaphoreType.DMA
    any_spec = pl.BlockSpec(memory_space=pl.ANY)
    vmem = pl.BlockSpec(memory_space=pltpu.VMEM)
    return pl.pallas_call(
        spread_kernel,
        out_shape=(
            jax.ShapeDtypeStruct((groups * width, half), BF16),
            jax.ShapeDtypeStruct((groups, 2, senders, most, width), BF16),
            jax.ShapeDtypeStruct((2, rows, half), BF16),
        ),
        in_specs=[vmem, any_spec],
        out_specs=(vmem, any_spec, any_spec),
        scratch_shapes=[
            pltpu.VMEM((groups, 2, senders, most, width), BF16),
            pltpu.VMEM((2, rows, half), BF16),
            dma((senders,)), dma((senders,)), dma((senders,)), dma((senders,)),
            dma((2, senders)), dma((2, senders)), dma((2, 2, senders)), dma((2, 2, senders)),
            dma((2,)), dma((1,)), dma((groups,)),
        ],
        compiler_params=pltpu.CompilerParams(
            collective_id=0, has_side_effects=True, vmem_limit_bytes=56 * 1024 * 1024
        ),
        cost_estimate=pl.CostEstimate(
            flops=60 * 10**9, bytes_accessed=32 * rows * half, transcendentals=0
        ),
        name="spread",
    )(outgoing, embed_grad)


def finish_kernel(
    n_ref, w_ref, eg_ref, emb_ref, t_ref,
    nv, dv, ra, yb, xb, rb, ev, a_s, a_r, b_s, b_r, c_s, c_r, t_s, t_r, e_sem, n_sem, l_sem,
):
    at = Place()
    senders, most, width = t_ref.shape
    rows, half = eg_ref.shape[1:]
    e, k, y, x, c = at.e, at.k, at.y, at.x, at.c
    ox, oy, ok = 1 - x, 1 - y, 1 - k
    c_y = at.group(k, oy)

    def load(w):
        return pltpu.make_async_copy(n_ref.at[:, w], nv, n_sem.at[0])

    load(ox).start()
    at.greet()

    def over(fn):
        lax.fori_loop(0, senders, lambda i, carry: (fn(i), carry)[1], 0)

    def product(group):
        for w in range(2):
            total = lax.dot_general(
                eg_ref[w], w_ref[group], (((1,), (1,)), ((), ())), preferred_element_type=F32
            )
            dv[group, w] = total.astype(BF16).reshape(senders, most, width)

    def core(v, s):
        return send(
            dv.at[at.group(ok, v), :, s], ra.at[v, :, s], a_s.at[v, s], a_r.at[v, s], at.k_peer
        )

    product(at.group(ok, oy))
    over(lambda s: core(oy, s).start())
    product(c_y)

    def across(s):
        return send(dv.at[c_y, :, s], yb.at[:, s], b_s.at[s], b_r.at[s], at.y_peer)

    def fold_core(s):
        core(oy, s).wait_recv()
        dv[c_y, :, s] = (dv[c_y, :, s].astype(F32) + ra[oy, :, s].astype(F32)).astype(BF16)
        across(s).start()

    over(fold_core)
    product(at.group(ok, y))
    over(lambda s: core(y, s).start())
    product(c)

    def embed(w):
        total = None
        for group in range(w_ref.shape[0]):
            term = jnp.dot(
                nv[group].reshape(rows, width), w_ref[group], preferred_element_type=F32
            )
            total = term if total is None else total + term
        return total.astype(BF16)

    own_cols = pl.ds(pl.multiple_of(x * half, LANES), half)
    load(ox).wait()
    ev[0] = embed(ox)
    load(x).start()
    emb_send = send(ev.at[0], emb_ref.at[:, own_cols], e_sem.at[0], e_sem.at[1], at.x_peer)

    def to_x(s):
        return send(dv.at[c, ox, s], xb.at[s], c_s.at[s], c_r.at[s], at.x_peer)

    def fold_y(s):
        core(y, s).wait_recv()
        across(s).wait_recv()
        dv[c, :, s] = (
            dv[c, :, s].astype(F32) + ra[y, :, s].astype(F32) + yb[:, s].astype(F32)
        ).astype(BF16)
        to_x(s).start()

    def back(s):
        return send(rb.at[s], t_ref.at[e], t_s.at[s], t_r.at[e], (s, k, y))

    def fold_x(s):
        to_x(s).wait_recv()
        rb[s] = (dv[c, x, s].astype(F32) + xb[s].astype(F32)).astype(BF16)

        @pl.when(s == e)
        def _():
            t_ref[e] = rb[e]

        @pl.when(s != e)
        def _():
            back(s).start()

    load(x).wait()
    ev[1] = embed(x)
    keep = pltpu.make_async_copy(ev.at[1], emb_ref.at[:, own_cols], l_sem.at[0])
    keep.start()

    fold_y(0)
    emb_send.start()

    def step(s):
        fold_y(s)
        fold_x(s - 1)

    lax.fori_loop(1, senders, lambda i, carry: (step(i), carry)[1], 0)
    fold_x(senders - 1)

    def came(i):
        s = at.other(i)
        send(rb.at[s], t_ref.at[s], t_s.at[s], t_r.at[s], (s, k, y)).wait_recv()
        back(s).wait_send()

    lax.fori_loop(1, senders, lambda i, carry: (came(i), carry)[1], 0)

    def sent(s):
        core(oy, s).wait_send()
        core(y, s).wait_send()
        across(s).wait_send()
        to_x(s).wait_send()

    over(sent)
    emb_send.wait_send()
    send(
        ev.at[0], emb_ref.at[:, pl.ds(pl.multiple_of(ox * half, LANES), half)], e_sem.at[0], e_sem.at[1], at.x_peer
    ).wait_recv()
    keep.wait()


def finish(shared, weight, grads):
    groups, _, senders, most, width = shared.shape
    _, rows, half = grads.shape
    dma = pltpu.SemaphoreType.DMA
    any_spec = pl.BlockSpec(memory_space=pl.ANY)
    vmem = pl.BlockSpec(memory_space=pltpu.VMEM)
    return pl.pallas_call(
        finish_kernel,
        out_shape=(
            jax.ShapeDtypeStruct((rows, 2 * half), BF16),
            jax.ShapeDtypeStruct((senders, most, width), BF16),
        ),
        in_specs=[any_spec, vmem, vmem],
        out_specs=(any_spec, vmem),
        scratch_shapes=[
            pltpu.VMEM((groups, senders, most, width), BF16),
            pltpu.VMEM((groups, 2, senders, most, width), BF16),
            pltpu.VMEM((2, 2, senders, most, width), BF16),
            pltpu.VMEM((2, senders, most, width), BF16),
            pltpu.VMEM((senders, most, width), BF16),
            pltpu.VMEM((senders, most, width), BF16),
            pltpu.VMEM((2, rows, half), BF16),
            dma((2, senders)), dma((2, senders)), dma((senders,)), dma((senders,)),
            dma((senders,)), dma((senders,)), dma((senders,)), dma((senders,)),
            dma((2,)), dma((1,)), dma((1,)),
        ],
        compiler_params=pltpu.CompilerParams(
            collective_id=1, has_side_effects=True, vmem_limit_bytes=62 * 1024 * 1024
        ),
        cost_estimate=pl.CostEstimate(
            flops=60 * 10**9, bytes_accessed=32 * rows * half, transcendentals=0
        ),
        name="finish",
    )(shared, weight, grads)


def owner_body(patches, gain, shift, proj_weight, llm_rank, embed_grad):
    features = ("section", "llmdp")
    own_rows, owned_width = patches.shape
    width = gain.shape[0]
    senders = lax.axis_size("enc")
    most_slots = embed_grad.shape[0] // senders
    block = 2
    near = [[b * block + i for i in range(block)] for b in range(senders // block)]
    far = [[b * block + i for b in range(senders // block)] for i in range(block)]

    def near_exchange(v, split, concat):
        return lax.all_to_all(v, "enc", split, concat, axis_index_groups=near, tiled=True)

    weight_part = near_exchange(proj_weight, 1, 0)
    weight = lax.all_gather(weight_part, "enc", axis=0, axis_index_groups=far, tiled=True)

    column_start = lax.axis_index(features) * owned_width
    gain_own = lax.dynamic_slice_in_dim(gain, column_start, owned_width, 0)
    shift_own = lax.dynamic_slice_in_dim(shift, column_start, owned_width, 0)
    values = patches.astype(F32)
    total, squares = lax.psum((jnp.sum(values, 1), jnp.sum(values * values, 1)), features)
    average = (total / width)[:, None]
    variance = (squares / width)[:, None] - average * average
    deviation = lax.rsqrt(variance + EPSILON)
    standardized = (values - average) * deviation
    normed = (standardized * gain_own + shift_own).astype(BF16)

    slot = slots_of(llm_rank, senders, most_slots)
    places = jnp.arange(senders * most_slots, dtype=jnp.int32)
    chosen = (places[:, None] == slot[None, :]).astype(BF16)
    outgoing = jnp.dot(chosen, normed, preferred_element_type=F32).astype(BF16)
    grad_partial, shared, grads = spread(
        outgoing.reshape(senders, most_slots, owned_width), embed_grad
    )
    grad_part = lax.psum_scatter(
        grad_partial, "enc", scatter_dimension=0, axis_index_groups=far, tiled=True
    )
    grad_weight = near_exchange(grad_part, 0, 1).astype(F32)

    embeds_recv, returned = finish(
        shared, weight.reshape(width // owned_width, owned_width, weight.shape[1]), grads
    )
    dnormed = lax.dot_general(
        chosen, returned.reshape(senders * most_slots, owned_width), (((0,), (0,)), ((), ())),
        preferred_element_type=F32,
    )
    dxhat = dnormed * gain_own
    mean_sum, cross_sum = lax.psum(
        (jnp.sum(dxhat, 1), jnp.sum(dxhat * standardized, 1)), features
    )
    hidden_state_gradient = (
        deviation
        * (dxhat - (mean_sum / width)[:, None] - standardized * (cross_sum / width)[:, None])
    ).astype(BF16)
    gain_gradient, grad_shift = lax.psum(
        (jnp.sum(dnormed * standardized, 0), jnp.sum(dnormed, 0)), "enc"
    )
    return (embeds_recv, hidden_state_gradient, grad_weight, gain_gradient, grad_shift)


def plain_body(patches, gain, shift, proj_weight, llm_rank, embed_grad):
    features = ("section", "llmdp")
    own_rows, owned_width = patches.shape
    width = gain.shape[0]
    weight_rows, out_cols = proj_weight.shape
    senders = lax.axis_size("enc")
    block = block_size(senders, out_cols)
    near = [[b * block + i for i in range(block)] for b in range(senders // block)]
    far = [[b * block + i for b in range(senders // block)] for i in range(block)]

    def near_exchange(x, split, concat):
        return lax.all_to_all(x, "enc", split, concat, axis_index_groups=near, tiled=True)

    column_start = lax.axis_index(features) * owned_width
    gain_own = lax.dynamic_slice_in_dim(gain, column_start, owned_width, 0)

    weight_part = near_exchange(proj_weight, 1, 0)
    weight = lax.all_gather(weight_part, "enc", axis=0, axis_index_groups=far, tiled=True)

    block_rows = lax.all_gather(patches, "enc", axis=0, axis_index_groups=near, tiled=True)
    complete_rows = lax.all_gather(block_rows, features, axis=1, tiled=True).astype(jnp.float32)
    row_average = jnp.mean(complete_rows, 1, keepdims=True)
    variance = jnp.mean(complete_rows * complete_rows, 1, keepdims=True) - row_average * row_average
    inverse_deviation = lax.rsqrt(variance + EPSILON)
    standardized = (complete_rows - row_average) * inverse_deviation
    normed = (standardized * gain + shift).astype(jnp.bfloat16)

    row_start = (lax.axis_index("enc") % block) * own_rows
    average_own = lax.dynamic_slice_in_dim(row_average, row_start, own_rows, 0)
    deviation_own = lax.dynamic_slice_in_dim(inverse_deviation, row_start, own_rows, 0)
    standardized_owned = (patches.astype(jnp.float32) - average_own) * deviation_own

    most_slots = embed_grad.shape[0] // senders
    target = llm_rank[:, 0]
    owners = jnp.arange(senders, dtype=jnp.int32)
    hits = (target[:, None] == owners[None, :]).astype(jnp.int32)
    rank = jnp.sum((jnp.cumsum(hits, 0) - hits) * hits, 1)
    slot = target * most_slots + rank

    def enc_exchange(x):
        return lax.all_to_all(
            x.reshape(senders, most_slots, out_cols), "enc", split_axis=0, concat_axis=0, tiled=True
        ).reshape(senders * most_slots, out_cols)

    d_embed = near_exchange(enc_exchange(embed_grad)[slot], 1, 0)
    grad_part = lax.psum_scatter(
        lax.dot_general(
            normed, d_embed, (((0,), (0,)), ((), ())), preferred_element_type=jnp.float32
        ).astype(jnp.bfloat16),
        "enc",
        scatter_dimension=0,
        axis_index_groups=far,
        tiled=True,
    )
    grad_weight = near_exchange(grad_part, 0, 1).astype(jnp.float32)

    embed_part = jnp.dot(normed, weight, preferred_element_type=jnp.float32).astype(jnp.bfloat16)
    embed = near_exchange(embed_part, 0, 1)
    outgoing = jnp.zeros((senders * most_slots, out_cols), jnp.bfloat16).at[slot].set(embed)
    embeds_recv = enc_exchange(outgoing)

    partial_grad = lax.dot_general(
        d_embed, weight, (((1,), (1,)), ((), ())), preferred_element_type=jnp.float32
    )
    group_count = width // owned_width
    pieces = partial_grad.astype(jnp.bfloat16).reshape(block * own_rows, group_count, owned_width)
    columns = lax.all_to_all(pieces, features, split_axis=1, concat_axis=1, tiled=True)
    column_sum = jnp.sum(columns.astype(jnp.float32), 1).astype(jnp.bfloat16)
    shares = near_exchange(column_sum.reshape(block, own_rows, owned_width), 0, 0)
    owned_normalized_gradient = jnp.sum(shares.astype(jnp.float32), 0)
    owned_centered_gradient = owned_normalized_gradient * gain_own
    mean_sum, cross_sum = lax.psum(
        (
            jnp.sum(owned_centered_gradient, 1),
            jnp.sum(owned_centered_gradient * standardized_owned, 1),
        ),
        features,
    )
    gradient_row_average = (mean_sum / width)[:, None]
    gradient_cross_product = (cross_sum / width)[:, None]
    hidden_state_gradient = (
        deviation_own
        * (
            owned_centered_gradient
            - gradient_row_average
            - standardized_owned * gradient_cross_product
        )
    ).astype(jnp.bfloat16)
    gain_gradient, grad_shift = lax.psum(
        (
            jnp.sum(owned_normalized_gradient * standardized_owned, 0),
            jnp.sum(owned_normalized_gradient, 0),
        ),
        "enc",
    )
    return (embeds_recv, hidden_state_gradient, grad_weight, gain_gradient, grad_shift)


def fits(patches, gain, proj_weight, embed_grad):
    senders, cores, rows_of = (lax.axis_size(a) for a in ("enc", "section", "llmdp"))
    most = embed_grad.shape[0] // senders
    return (
        cores == 2
        and rows_of == 2
        and block_size(senders, proj_weight.shape[1]) == 2
        and senders // 2 == cores * rows_of
        and most % SUBLANES == 0
        and proj_weight.shape[0] % SUBLANES == 0
        and patches.shape[1] == 2 * proj_weight.shape[0]
    )


def body(patches, gain, shift, proj_weight, llm_rank, embed_grad):
    form = owner_body if fits(patches, gain, proj_weight, embed_grad) else plain_body
    return form(patches, gain, shift, proj_weight, llm_rank, embed_grad)


def solution(mesh):
    in_specs = (
        P("enc", ("section", "llmdp")),
        P(),
        P(),
        P("enc", ("section", "llmdp")),
        P("enc", None),
        P("enc", ("section", "llmdp")),
    )
    out_specs = (
        P("enc", ("section", "llmdp")),
        P("enc", ("section", "llmdp")),
        P("enc", ("section", "llmdp")),
        P(("section", "llmdp")),
        P(("section", "llmdp")),
    )
    return jax.shard_map(body, mesh=mesh, in_specs=in_specs, out_specs=out_specs, check_vma=False)
```

```python
import functools

import jax
import jax.numpy as jnp
from jax import lax
from jax.experimental import pallas as pl
from jax.experimental.pallas import tpu as pltpu
from jax.sharding import PartitionSpec as P

EPSILON = 1e-05
MESH = pl.DeviceIdType.MESH
F32 = jnp.float32
BF16 = jnp.bfloat16

MAX_BLOCK = 2
SUBLANES = 16
LANES = 128


def block_size(senders, out_cols):
    size = MAX_BLOCK
    while size > 1 and (senders % size or senders == size or out_cols % (size * 128)):
        size //= 2
    return size


def slots_of(llm_rank, senders, most_slots):
    target = llm_rank[:, 0]
    owners = jnp.arange(senders, dtype=jnp.int32)
    hits = (target[:, None] == owners[None, :]).astype(jnp.int32)
    rank = jnp.sum((jnp.cumsum(hits, 0) - hits) * hits, 1)
    return target * most_slots + rank


class Place:
    def __init__(self):
        self.e = lax.axis_index("enc")
        self.k = lax.axis_index("section")
        self.y = lax.axis_index("llmdp")
        self.x = lax.rem(self.e, 2)
        self.senders = lax.axis_size("enc")
        self.c = self.group(self.k, self.y)
        self.x_peer = (self.e + 1 - 2 * self.x, self.k, self.y)
        self.y_peer = (self.e, self.k, 1 - self.y)
        self.k_peer = (self.e, 1 - self.k, self.y)

    def group(self, k, y):
        return k * 2 + y

    def other(self, step):
        return lax.rem(self.e + step, self.senders)

    def greet(self):
        barrier = pltpu.get_barrier_semaphore()

        def one(step, carry):
            pl.semaphore_signal(
                barrier, inc=1, device_id=(self.other(step), self.k, self.y), device_id_type=MESH
            )
            return carry

        lax.fori_loop(1, self.senders, one, 0)
        for peer in (self.y_peer, self.k_peer):
            pl.semaphore_signal(barrier, inc=1, device_id=peer, device_id_type=MESH)
        pl.semaphore_wait(barrier, self.senders + 1)


def send(src, dst, send_sem, recv_sem, device):
    return pltpu.make_async_remote_copy(
        src_ref=src, dst_ref=dst, send_sem=send_sem, recv_sem=recv_sem, device_id=device, device_id_type=MESH
    )


def spread_kernel(
    out_ref, eg_ref, w_ref, gw_ref, n_ref, eg_out, wg_ref,
    nv, eg_v, wl, route_s, route_r, x_s, x_r, y_s, y_r, d_s, d_r, eg_sem, local_sem, n_sem, w_x, w_s, w_r,
):
    at = Place()
    senders, most, width = out_ref.shape
    half = eg_v.shape[2]
    rows = eg_v.shape[1]
    groups = nv.shape[0]
    e, k, y, x, c = at.e, at.k, at.y, at.x, at.c
    ox = 1 - x
    c_y, c_k, c_ky = at.group(k, 1 - y), at.group(1 - k, y), at.group(1 - k, 1 - y)

    def route(d):
        return send(out_ref.at[d], nv.at[c, lax.rem(d, 2), e], route_s.at[d], route_r.at[e], (d, k, y))

    def route_in(s):
        return send(out_ref.at[s], nv.at[c, x, s], route_s.at[s], route_r.at[s], (s, k, y))

    def x_hop(s, src):
        return send(src, nv.at[c, x, s], x_s.at[s], x_r.at[s], at.x_peer)

    def x_in(s):
        return send(nv.at[c, ox, s], nv.at[c, ox, s], x_s.at[s], x_r.at[s], at.x_peer)

    def y_hop(w, s, src):
        return send(src, nv.at[c, w, s], y_s.at[w, s], y_r.at[w, s], at.y_peer)

    def y_in(w, s):
        return send(nv.at[c_y, w, s], nv.at[c_y, w, s], y_s.at[w, s], y_r.at[w, s], at.y_peer)

    def k_hop(v, w, s, src):
        return send(src, nv.at[at.group(k, v), w, s], d_s.at[v, w, s], d_r.at[v, w, s], at.k_peer)

    def k_in(v, w, s):
        ref = nv.at[at.group(1 - k, v), w, s]
        return send(ref, ref, d_s.at[v, w, s], d_r.at[v, w, s], at.k_peer)

    eg_send = send(
        eg_ref.at[:, pl.ds(pl.multiple_of(ox * half, LANES), half)], eg_v.at[x], eg_sem.at[0], eg_sem.at[1], at.x_peer
    )
    eg_load = pltpu.make_async_copy(
        eg_ref.at[:, pl.ds(pl.multiple_of(x * half, LANES), half)], eg_v.at[x], local_sem.at[0]
    )
    eg_in = send(eg_v.at[ox], eg_v.at[ox], eg_sem.at[0], eg_sem.at[1], at.x_peer)

    eg_load.start()
    own_half = pl.ds(pl.multiple_of(x * half, LANES), half)
    peer_half = pl.ds(pl.multiple_of(ox * half, LANES), half)
    w_load = pltpu.make_async_copy(w_ref.at[:, own_half], wl, local_sem.at[1])
    w_keep = pltpu.make_async_copy(wl, wg_ref.at[e], local_sem.at[2])
    w_load.start()
    z = e // 2
    e_peer = e + 1 - 2 * x
    w_swap = send(w_ref.at[:, peer_half], wg_ref.at[e], w_x.at[0], w_x.at[1], at.x_peer)
    w_swap_in = send(wg_ref.at[e_peer], wg_ref.at[e_peer], w_x.at[0], w_x.at[1], at.x_peer)

    def w_hop(b, src, way):
        to = e + 2 if way == 0 else e - 2
        return send(src, wg_ref.at[b], w_s.at[way, b], w_r.at[b], (to, k, y))

    def room(way, distance):
        if way == 0:
            return (z >= distance) & (z + 1 < senders // 2)
        return (z + distance < senders // 2) & (z >= 1)

    def came(way, distance):
        return z >= distance if way == 0 else z + distance < senders // 2

    def block_from(way, distance, parity):
        return 2 * (z - distance if way == 0 else z + distance) + parity

    def w_own(b, src):
        for way in range(2):
            @pl.when(room(way, 0))
            def _():
                w_hop(b, src, way).start()

    def w_relay(distance):
        for parity in (x, ox):
            for way in range(2):
                @pl.when(came(way, distance))
                def _():
                    b = block_from(way, distance, parity)
                    w_hop(b, wg_ref.at[b], way).wait_recv()

                    @pl.when(room(way, distance))
                    def _():
                        w_hop(b, wg_ref.at[b], way).start()

    def w_sent(distance):
        for parity in (x, ox):
            for way in range(2):
                @pl.when(room(way, distance))
                def _():
                    b = block_from(way, distance, parity)
                    w_hop(b, wg_ref.at[b], way).wait_send()

    at.greet()

    def over(fn, start=0):
        lax.fori_loop(start, senders, lambda i, carry: (fn(i), carry)[1], 0)

    over(lambda step: route(at.other(step)).start(), 1)
    own = out_ref.at[e]
    x_hop(e, own).start()
    y_hop(x, e, own).start()
    k_hop(y, x, e, own).start()
    w_swap.start()
    w_load.wait()
    w_own(e, wl)
    w_keep.start()
    nv[c, x, e] = out_ref[e]

    def pass_on(step):
        s = at.other(step)
        ref = nv.at[c, x, s]
        route_in(s).wait_recv()
        x_hop(s, ref).start()
        y_hop(x, s, ref).start()
        k_hop(y, x, s, ref).start()

    over(pass_on, 1)
    eg_send.start()
    w_swap_in.wait_recv()
    w_own(e_peer, wg_ref.at[e_peer])

    def pass_x(step):
        s = at.other(step)
        ref = nv.at[c, ox, s]
        x_in(s).wait_recv()
        y_hop(ox, s, ref).start()
        k_hop(y, ox, s, ref).start()

    over(pass_x)
    w_relay(1)

    def product(group):
        total = None
        for w in range(2):
            term = lax.dot_general(
                nv[group, w].reshape(rows, width), eg_v[w], (((0,), (0,)), ((), ())), preferred_element_type=F32
            )
            total = term if total is None else total + term
        gw_ref[pl.ds(pl.multiple_of(group * width, SUBLANES), width), :] = total.astype(BF16)

    def keep(i, group):
        pltpu.make_async_copy(nv.at[group], n_ref.at[group], n_sem.at[i]).start()

    def pass_y(w):
        def one(step):
            s = at.other(step)
            y_in(w, s).wait_recv()
            k_hop(1 - y, w, s, nv.at[c_y, w, s]).start()

        over(one)

    keep(0, c)
    eg_load.wait()
    eg_in.wait_recv()
    eg_keep = pltpu.make_async_copy(eg_v, eg_out, local_sem.at[0])
    eg_keep.start()
    product(c)
    pass_y(x)

    def near_in(step):
        for w in range(2):
            k_in(y, w, at.other(step)).wait_recv()

    over(near_in)
    keep(1, c_k)
    product(c_k)
    pass_y(ox)
    w_relay(2)
    keep(2, c_y)
    product(c_y)

    def far_in(step):
        for w in range(2):
            k_in(1 - y, w, at.other(step)).wait_recv()

    over(far_in)
    keep(3, c_ky)
    product(c_ky)

    for distance in range(3, groups):
        w_relay(distance)
    for distance in range(groups):
        w_sent(distance)
    w_swap.wait_send()
    w_keep.wait()
    over(lambda step: route(at.other(step)).wait_send(), 1)

    def sent(step):
        s = at.other(step)
        x_hop(s, nv.at[c, x, s]).wait_send()
        for w in range(2):
            y_hop(w, s, nv.at[c, w, s]).wait_send()
            for v in range(2):
                k_hop(v, w, s, nv.at[at.group(k, v), w, s]).wait_send()

    over(sent)
    eg_send.wait_send()
    eg_keep.wait()
    for i, group in enumerate((c, c_k, c_y, c_ky)):
        pltpu.make_async_copy(nv.at[group], n_ref.at[group], n_sem.at[i]).wait()


def spread(outgoing, embed_grad, proj_weight):
    senders, most, width = outgoing.shape
    groups = 4
    rows, cols = embed_grad.shape
    half = cols // 2
    dma = pltpu.SemaphoreType.DMA
    any_spec = pl.BlockSpec(memory_space=pl.ANY)
    vmem = pl.BlockSpec(memory_space=pltpu.VMEM)
    return pl.pallas_call(
        spread_kernel,
        out_shape=(
            jax.ShapeDtypeStruct((groups * width, half), BF16),
            jax.ShapeDtypeStruct((groups, 2, senders, most, width), BF16),
            jax.ShapeDtypeStruct((2, rows, half), BF16),
            jax.ShapeDtypeStruct((senders, proj_weight.shape[0], half), BF16),
        ),
        in_specs=[vmem, any_spec, any_spec],
        out_specs=(vmem, any_spec, any_spec, any_spec),
        scratch_shapes=[
            pltpu.VMEM((groups, 2, senders, most, width), BF16),
            pltpu.VMEM((2, rows, half), BF16),
            pltpu.VMEM((proj_weight.shape[0], half), BF16),
            dma((senders,)), dma((senders,)), dma((senders,)), dma((senders,)),
            dma((2, senders)), dma((2, senders)), dma((2, 2, senders)), dma((2, 2, senders)),
            dma((2,)), dma((3,)), dma((groups,)), dma((2,)), dma((2, senders)), dma((senders,)),
        ],
        compiler_params=pltpu.CompilerParams(
            collective_id=0, has_side_effects=True, vmem_limit_bytes=56 * 1024 * 1024
        ),
        cost_estimate=pl.CostEstimate(
            flops=60 * 10**9, bytes_accessed=32 * rows * half, transcendentals=0
        ),
        name="spread",
    )(outgoing, embed_grad, proj_weight)


def finish_kernel(
    n_ref, w_ref, eg_ref, emb_ref, t_ref,
    nv, dv, ra, yb, xb, rb, ev, a_s, a_r, b_s, b_r, c_s, c_r, t_s, t_r, e_sem, n_sem, l_sem,
):
    at = Place()
    senders, most, width = t_ref.shape
    rows, half = eg_ref.shape[1:]
    e, k, y, x, c = at.e, at.k, at.y, at.x, at.c
    ox, oy, ok = 1 - x, 1 - y, 1 - k
    c_y = at.group(k, oy)

    def load(w):
        return pltpu.make_async_copy(n_ref.at[:, w], nv, n_sem.at[0])

    load(ox).start()
    at.greet()

    def over(fn):
        lax.fori_loop(0, senders, lambda i, carry: (fn(i), carry)[1], 0)

    def product(group):
        def one(w, carry):
            total = lax.dot_general(
                eg_ref[w], w_ref[group], (((1,), (1,)), ((), ())), preferred_element_type=F32
            )
            dv[group, w] = total.astype(BF16).reshape(senders, most, width)
            return carry

        lax.fori_loop(0, 2, one, 0)

    def core(v, s):
        return send(
            dv.at[at.group(ok, v), :, s], ra.at[v, :, s], a_s.at[v, s], a_r.at[v, s], at.k_peer
        )

    product(at.group(ok, oy))
    over(lambda s: core(oy, s).start())
    product(c_y)

    def across(s):
        return send(dv.at[c_y, :, s], yb.at[:, s], b_s.at[s], b_r.at[s], at.y_peer)

    def fold_core(s):
        core(oy, s).wait_recv()
        dv[c_y, :, s] = (dv[c_y, :, s].astype(F32) + ra[oy, :, s].astype(F32)).astype(BF16)
        across(s).start()

    over(fold_core)
    product(at.group(ok, y))
    over(lambda s: core(y, s).start())
    product(c)

    def embed(w):
        total = None
        for group in range(w_ref.shape[0]):
            term = jnp.dot(
                nv[group].reshape(rows, width), w_ref[group], preferred_element_type=F32
            )
            total = term if total is None else total + term
        return total.astype(BF16)

    own_cols = pl.ds(pl.multiple_of(x * half, LANES), half)
    load(ox).wait()
    ev[0] = embed(ox)
    load(x).start()
    emb_send = send(ev.at[0], emb_ref.at[:, own_cols], e_sem.at[0], e_sem.at[1], at.x_peer)

    def to_x(s):
        return send(dv.at[c, ox, s], xb.at[s], c_s.at[s], c_r.at[s], at.x_peer)

    def fold_y(s):
        core(y, s).wait_recv()
        across(s).wait_recv()
        dv[c, :, s] = (
            dv[c, :, s].astype(F32) + ra[y, :, s].astype(F32) + yb[:, s].astype(F32)
        ).astype(BF16)
        to_x(s).start()

    def back(s):
        return send(rb.at[s], t_ref.at[e], t_s.at[s], t_r.at[e], (s, k, y))

    def fold_x(s):
        to_x(s).wait_recv()
        rb[s] = (dv[c, x, s].astype(F32) + xb[s].astype(F32)).astype(BF16)

        @pl.when(s == e)
        def _():
            t_ref[e] = rb[e]

        @pl.when(s != e)
        def _():
            back(s).start()

    load(x).wait()
    ev[1] = embed(x)
    keep = pltpu.make_async_copy(ev.at[1], emb_ref.at[:, own_cols], l_sem.at[0])
    keep.start()

    fold_y(0)
    emb_send.start()

    def step(s):
        fold_y(s)
        fold_x(s - 1)

    lax.fori_loop(1, senders, lambda i, carry: (step(i), carry)[1], 0)
    fold_x(senders - 1)

    def came(i):
        s = at.other(i)
        send(rb.at[s], t_ref.at[s], t_s.at[s], t_r.at[s], (s, k, y)).wait_recv()
        back(s).wait_send()

    lax.fori_loop(1, senders, lambda i, carry: (came(i), carry)[1], 0)

    def sent(s):
        core(oy, s).wait_send()
        core(y, s).wait_send()
        across(s).wait_send()
        to_x(s).wait_send()

    over(sent)
    emb_send.wait_send()
    send(
        ev.at[0], emb_ref.at[:, pl.ds(pl.multiple_of(ox * half, LANES), half)], e_sem.at[0], e_sem.at[1], at.x_peer
    ).wait_recv()
    keep.wait()


def finish(shared, weight, grads):
    groups, _, senders, most, width = shared.shape
    _, rows, half = grads.shape
    dma = pltpu.SemaphoreType.DMA
    any_spec = pl.BlockSpec(memory_space=pl.ANY)
    vmem = pl.BlockSpec(memory_space=pltpu.VMEM)
    return pl.pallas_call(
        finish_kernel,
        out_shape=(
            jax.ShapeDtypeStruct((rows, 2 * half), BF16),
            jax.ShapeDtypeStruct((senders, most, width), BF16),
        ),
        in_specs=[any_spec, vmem, vmem],
        out_specs=(any_spec, vmem),
        scratch_shapes=[
            pltpu.VMEM((groups, senders, most, width), BF16),
            pltpu.VMEM((groups, 2, senders, most, width), BF16),
            pltpu.VMEM((2, 2, senders, most, width), BF16),
            pltpu.VMEM((2, senders, most, width), BF16),
            pltpu.VMEM((senders, most, width), BF16),
            pltpu.VMEM((senders, most, width), BF16),
            pltpu.VMEM((2, rows, half), BF16),
            dma((2, senders)), dma((2, senders)), dma((senders,)), dma((senders,)),
            dma((senders,)), dma((senders,)), dma((senders,)), dma((senders,)),
            dma((2,)), dma((1,)), dma((1,)),
        ],
        compiler_params=pltpu.CompilerParams(
            collective_id=1, has_side_effects=True, vmem_limit_bytes=62 * 1024 * 1024
        ),
        cost_estimate=pl.CostEstimate(
            flops=60 * 10**9, bytes_accessed=32 * rows * half, transcendentals=0
        ),
        name="finish",
    )(shared, weight, grads)


def row_kernel(mine, total, seen, send_sem, recv_sem):
    at = Place()
    groups = seen.shape[0]
    peers = [(k, y) for k in range(2) for y in range(2)]
    barrier = pltpu.get_barrier_semaphore()

    def others(fn):
        for k, y in peers:
            @pl.when(at.group(k, y) != at.c)
            def _():
                fn(k, y)

    others(
        lambda k, y: pl.semaphore_signal(barrier, inc=1, device_id=(at.e, k, y), device_id_type=MESH)
    )
    pl.semaphore_wait(barrier, groups - 1)

    def copy(k, y, slot):
        g = at.group(k, y)
        return send(mine, seen.at[slot], send_sem.at[g], recv_sem.at[slot], (at.e, k, y))

    others(lambda k, y: copy(k, y, at.c).start())
    seen[at.c] = mine[...]
    others(lambda k, y: copy(k, y, at.group(k, y)).wait_recv())
    result = seen[0]
    for g in range(1, groups):
        result = result + seen[g]
    total[...] = result
    others(lambda k, y: copy(k, y, at.c).wait_send())


def sum_rows(rows, groups):
    vmem = pl.BlockSpec(memory_space=pltpu.VMEM)
    return pl.pallas_call(
        row_kernel,
        out_shape=jax.ShapeDtypeStruct(rows.shape, F32),
        in_specs=[vmem],
        out_specs=vmem,
        scratch_shapes=[
            pltpu.VMEM((groups, *rows.shape), F32),
            pltpu.SemaphoreType.DMA((groups,)),
            pltpu.SemaphoreType.DMA((groups,)),
        ],
        compiler_params=pltpu.CompilerParams(collective_id=2, has_side_effects=True),
        name="sum_rows",
    )(rows)


def both_kernel(mine, mine_cols, total, total_cols, seen, seen_cols, r_s, r_r, c_s, c_r):
    at = Place()
    groups, senders = seen.shape[0], seen_cols.shape[0]
    peers = [(k, y) for k in range(2) for y in range(2)]
    barrier = pltpu.get_barrier_semaphore()

    def others(fn):
        for k, y in peers:
            @pl.when(at.group(k, y) != at.c)
            def _():
                fn(k, y)

    def along(fn):
        lax.fori_loop(1, senders, lambda i, carry: (fn(at.other(i)), carry)[1], 0)

    def signal(device):
        pl.semaphore_signal(barrier, inc=1, device_id=device, device_id_type=MESH)

    others(lambda k, y: signal((at.e, k, y)))
    along(lambda d: signal((d, at.k, at.y)))
    pl.semaphore_wait(barrier, groups + senders - 2)

    def copy(k, y, slot):
        g = at.group(k, y)
        return send(mine, seen.at[slot], r_s.at[g], r_r.at[slot], (at.e, k, y))

    def col(d, slot):
        return send(mine_cols, seen_cols.at[slot], c_s.at[d], c_r.at[slot], (d, at.k, at.y))

    others(lambda k, y: copy(k, y, at.c).start())
    along(lambda d: col(d, at.e).start())
    seen[at.c] = mine[...]
    seen_cols[at.e] = mine_cols[...]
    others(lambda k, y: copy(k, y, at.group(k, y)).wait_recv())
    along(lambda d: col(d, d).wait_recv())
    result = seen[0]
    for g in range(1, groups):
        result = result + seen[g]
    total[...] = result
    result = seen_cols[0]
    for d in range(1, senders):
        result = result + seen_cols[d]
    total_cols[...] = result
    others(lambda k, y: copy(k, y, at.c).wait_send())
    along(lambda d: col(d, at.e).wait_send())


def sum_both(rows, cols, groups, senders):
    vmem = pl.BlockSpec(memory_space=pltpu.VMEM)
    dma = pltpu.SemaphoreType.DMA
    return pl.pallas_call(
        both_kernel,
        out_shape=(
            jax.ShapeDtypeStruct(rows.shape, F32),
            jax.ShapeDtypeStruct(cols.shape, F32),
        ),
        in_specs=[vmem, vmem],
        out_specs=(vmem, vmem),
        scratch_shapes=[
            pltpu.VMEM((groups, *rows.shape), F32),
            pltpu.VMEM((senders, *cols.shape), F32),
            dma((groups,)), dma((groups,)), dma((senders,)), dma((senders,)),
        ],
        compiler_params=pltpu.CompilerParams(collective_id=3, has_side_effects=True),
        name="sum_both",
    )(rows, cols)


def owner_body(patches, gain, shift, proj_weight, llm_rank, embed_grad):
    features = ("section", "llmdp")
    own_rows, owned_width = patches.shape
    width = gain.shape[0]
    senders = lax.axis_size("enc")
    most_slots = embed_grad.shape[0] // senders
    block = 2
    near = [[b * block + i for i in range(block)] for b in range(senders // block)]
    far = [[b * block + i for b in range(senders // block)] for i in range(block)]

    def near_exchange(v, split, concat):
        return lax.all_to_all(v, "enc", split, concat, axis_index_groups=near, tiled=True)

    groups = width // owned_width
    column_start = lax.axis_index(features) * owned_width
    gain_own = lax.dynamic_slice_in_dim(gain, column_start, owned_width, 0)
    shift_own = lax.dynamic_slice_in_dim(shift, column_start, owned_width, 0)
    values = patches.astype(F32)
    total, squares = sum_rows(jnp.stack([jnp.sum(values, 1), jnp.sum(values * values, 1)]), groups)
    average = (total / width)[:, None]
    variance = (squares / width)[:, None] - average * average
    deviation = lax.rsqrt(variance + EPSILON)
    standardized = (values - average) * deviation
    normed = (standardized * gain_own + shift_own).astype(BF16)

    slot = slots_of(llm_rank, senders, most_slots)
    places = jnp.arange(senders * most_slots, dtype=jnp.int32)
    chosen = (places[:, None] == slot[None, :]).astype(BF16)
    outgoing = jnp.dot(chosen, normed, preferred_element_type=F32).astype(BF16)
    grad_partial, shared, grads, weight = spread(
        outgoing.reshape(senders, most_slots, owned_width), embed_grad, proj_weight
    )
    grad_part = lax.psum_scatter(
        grad_partial, "enc", scatter_dimension=0, axis_index_groups=far, tiled=True
    )
    grad_weight = near_exchange(grad_part, 0, 1).astype(F32)

    embeds_recv, returned = finish(
        shared, weight.reshape(groups, owned_width, weight.shape[2]), grads
    )
    dnormed = lax.dot_general(
        chosen, returned.reshape(senders * most_slots, owned_width), (((0,), (0,)), ((), ())),
        preferred_element_type=F32,
    )
    dxhat = dnormed * gain_own
    (mean_sum, cross_sum), (gain_gradient, grad_shift) = sum_both(
        jnp.stack([jnp.sum(dxhat, 1), jnp.sum(dxhat * standardized, 1)]),
        jnp.stack([jnp.sum(dnormed * standardized, 0), jnp.sum(dnormed, 0)]),
        groups,
        senders,
    )
    hidden_state_gradient = (
        deviation
        * (dxhat - (mean_sum / width)[:, None] - standardized * (cross_sum / width)[:, None])
    ).astype(BF16)
    return (embeds_recv, hidden_state_gradient, grad_weight, gain_gradient, grad_shift)


def plain_body(patches, gain, shift, proj_weight, llm_rank, embed_grad):
    features = ("section", "llmdp")
    own_rows, owned_width = patches.shape
    width = gain.shape[0]
    weight_rows, out_cols = proj_weight.shape
    senders = lax.axis_size("enc")
    block = block_size(senders, out_cols)
    near = [[b * block + i for i in range(block)] for b in range(senders // block)]
    far = [[b * block + i for b in range(senders // block)] for i in range(block)]

    def near_exchange(x, split, concat):
        return lax.all_to_all(x, "enc", split, concat, axis_index_groups=near, tiled=True)

    column_start = lax.axis_index(features) * owned_width
    gain_own = lax.dynamic_slice_in_dim(gain, column_start, owned_width, 0)

    weight_part = near_exchange(proj_weight, 1, 0)
    weight = lax.all_gather(weight_part, "enc", axis=0, axis_index_groups=far, tiled=True)

    block_rows = lax.all_gather(patches, "enc", axis=0, axis_index_groups=near, tiled=True)
    complete_rows = lax.all_gather(block_rows, features, axis=1, tiled=True).astype(jnp.float32)
    row_average = jnp.mean(complete_rows, 1, keepdims=True)
    variance = jnp.mean(complete_rows * complete_rows, 1, keepdims=True) - row_average * row_average
    inverse_deviation = lax.rsqrt(variance + EPSILON)
    standardized = (complete_rows - row_average) * inverse_deviation
    normed = (standardized * gain + shift).astype(jnp.bfloat16)

    row_start = (lax.axis_index("enc") % block) * own_rows
    average_own = lax.dynamic_slice_in_dim(row_average, row_start, own_rows, 0)
    deviation_own = lax.dynamic_slice_in_dim(inverse_deviation, row_start, own_rows, 0)
    standardized_owned = (patches.astype(jnp.float32) - average_own) * deviation_own

    most_slots = embed_grad.shape[0] // senders
    target = llm_rank[:, 0]
    owners = jnp.arange(senders, dtype=jnp.int32)
    hits = (target[:, None] == owners[None, :]).astype(jnp.int32)
    rank = jnp.sum((jnp.cumsum(hits, 0) - hits) * hits, 1)
    slot = target * most_slots + rank

    def enc_exchange(x):
        return lax.all_to_all(
            x.reshape(senders, most_slots, out_cols), "enc", split_axis=0, concat_axis=0, tiled=True
        ).reshape(senders * most_slots, out_cols)

    d_embed = near_exchange(enc_exchange(embed_grad)[slot], 1, 0)
    grad_part = lax.psum_scatter(
        lax.dot_general(
            normed, d_embed, (((0,), (0,)), ((), ())), preferred_element_type=jnp.float32
        ).astype(jnp.bfloat16),
        "enc",
        scatter_dimension=0,
        axis_index_groups=far,
        tiled=True,
    )
    grad_weight = near_exchange(grad_part, 0, 1).astype(jnp.float32)

    embed_part = jnp.dot(normed, weight, preferred_element_type=jnp.float32).astype(jnp.bfloat16)
    embed = near_exchange(embed_part, 0, 1)
    outgoing = jnp.zeros((senders * most_slots, out_cols), jnp.bfloat16).at[slot].set(embed)
    embeds_recv = enc_exchange(outgoing)

    partial_grad = lax.dot_general(
        d_embed, weight, (((1,), (1,)), ((), ())), preferred_element_type=jnp.float32
    )
    group_count = width // owned_width
    pieces = partial_grad.astype(jnp.bfloat16).reshape(block * own_rows, group_count, owned_width)
    columns = lax.all_to_all(pieces, features, split_axis=1, concat_axis=1, tiled=True)
    column_sum = jnp.sum(columns.astype(jnp.float32), 1).astype(jnp.bfloat16)
    shares = near_exchange(column_sum.reshape(block, own_rows, owned_width), 0, 0)
    owned_normalized_gradient = jnp.sum(shares.astype(jnp.float32), 0)
    owned_centered_gradient = owned_normalized_gradient * gain_own
    mean_sum, cross_sum = lax.psum(
        (
            jnp.sum(owned_centered_gradient, 1),
            jnp.sum(owned_centered_gradient * standardized_owned, 1),
        ),
        features,
    )
    gradient_row_average = (mean_sum / width)[:, None]
    gradient_cross_product = (cross_sum / width)[:, None]
    hidden_state_gradient = (
        deviation_own
        * (
            owned_centered_gradient
            - gradient_row_average
            - standardized_owned * gradient_cross_product
        )
    ).astype(jnp.bfloat16)
    gain_gradient, grad_shift = lax.psum(
        (
            jnp.sum(owned_normalized_gradient * standardized_owned, 0),
            jnp.sum(owned_normalized_gradient, 0),
        ),
        "enc",
    )
    return (embeds_recv, hidden_state_gradient, grad_weight, gain_gradient, grad_shift)


def fits(patches, gain, proj_weight, embed_grad):
    senders, cores, rows_of = (lax.axis_size(a) for a in ("enc", "section", "llmdp"))
    most = embed_grad.shape[0] // senders
    return (
        cores == 2
        and rows_of == 2
        and block_size(senders, proj_weight.shape[1]) == 2
        and senders // 2 == cores * rows_of
        and most % SUBLANES == 0
        and proj_weight.shape[0] % SUBLANES == 0
        and patches.shape[1] == 2 * proj_weight.shape[0]
    )


def body(patches, gain, shift, proj_weight, llm_rank, embed_grad):
    form = owner_body if fits(patches, gain, proj_weight, embed_grad) else plain_body
    return form(patches, gain, shift, proj_weight, llm_rank, embed_grad)


def solution(mesh):
    in_specs = (
        P("enc", ("section", "llmdp")),
        P(),
        P(),
        P("enc", ("section", "llmdp")),
        P("enc", None),
        P("enc", ("section", "llmdp")),
    )
    out_specs = (
        P("enc", ("section", "llmdp")),
        P("enc", ("section", "llmdp")),
        P("enc", ("section", "llmdp")),
        P(("section", "llmdp")),
        P(("section", "llmdp")),
    )
    return jax.shard_map(body, mesh=mesh, in_specs=in_specs, out_specs=out_specs, check_vma=False)
```

```python
import functools

import jax
import jax.numpy as jnp
from jax import lax
from jax.experimental import pallas as pl
from jax.experimental.pallas import tpu as pltpu
from jax.sharding import PartitionSpec as P

EPSILON = 1e-05
MESH = pl.DeviceIdType.MESH
F32 = jnp.float32
BF16 = jnp.bfloat16

MAX_BLOCK = 2
SUBLANES = 16
LANES = 128


def block_size(senders, out_cols):
    size = MAX_BLOCK
    while size > 1 and (senders % size or senders == size or out_cols % (size * 128)):
        size //= 2
    return size


def slots_of(llm_rank, senders, most_slots):
    target = llm_rank[:, 0]
    owners = jnp.arange(senders, dtype=jnp.int32)
    hits = (target[:, None] == owners[None, :]).astype(jnp.int32)
    rank = jnp.sum((jnp.cumsum(hits, 0) - hits) * hits, 1)
    return target * most_slots + rank


class Place:
    def __init__(self):
        self.e = lax.axis_index("enc")
        self.k = lax.axis_index("section")
        self.y = lax.axis_index("llmdp")
        self.x = lax.rem(self.e, 2)
        self.senders = lax.axis_size("enc")
        self.c = self.group(self.k, self.y)
        self.x_peer = (self.e + 1 - 2 * self.x, self.k, self.y)
        self.y_peer = (self.e, self.k, 1 - self.y)
        self.k_peer = (self.e, 1 - self.k, self.y)

    def group(self, k, y):
        return k * 2 + y

    def other(self, step):
        return lax.rem(self.e + step, self.senders)

    def greet(self):
        barrier = pltpu.get_barrier_semaphore()

        def one(step, carry):
            pl.semaphore_signal(
                barrier, inc=1, device_id=(self.other(step), self.k, self.y), device_id_type=MESH
            )
            return carry

        lax.fori_loop(1, self.senders, one, 0)
        for peer in (self.y_peer, self.k_peer):
            pl.semaphore_signal(barrier, inc=1, device_id=peer, device_id_type=MESH)
        pl.semaphore_wait(barrier, self.senders + 1)


def send(src, dst, send_sem, recv_sem, device):
    return pltpu.make_async_remote_copy(
        src_ref=src, dst_ref=dst, send_sem=send_sem, recv_sem=recv_sem, device_id=device, device_id_type=MESH
    )


def loop(count, fn, start=0):
    lax.fori_loop(start, count, lambda i, carry: (fn(i), carry)[1], 0)


class Line:
    def __init__(self, at):
        self.z = at.e // 2
        self.count = at.senders // 2
        self.parities = (at.x, 1 - at.x)

    def came(self, way, distance):
        return self.z >= distance if way == 0 else self.z + distance < self.count

    def room(self, way, distance):
        if way == 0:
            return (self.z >= distance) & (self.z + 1 < self.count)
        return (self.z + distance < self.count) & (self.z >= 1)

    def block(self, way, distance, parity):
        return 2 * (self.z - distance if way == 0 else self.z + distance) + parity

    def visit(self, distance, condition, fn):
        for parity in self.parities:
            for way in range(2):
                @pl.when(condition(way, distance))
                def _():
                    fn(way, self.block(way, distance, parity))


def spread_kernel(
    out_ref, eg_ref, w_ref, gw_ref, n_ref, eg_out, wg_ref,
    nv, eg_v, wl, route_s, route_r, x_s, x_r, y_s, y_r, d_s, d_r, eg_s, eg_r, local_sem, n_sem, w_x, w_s, w_r,
):
    at = Place()
    line = Line(at)
    senders, most, width = out_ref.shape
    rows, half = eg_v.shape[1:]
    groups = nv.shape[0]
    chips = senders // 2
    e, k, y, x, c, z = at.e, at.k, at.y, at.x, at.c, line.z
    ox = 1 - x
    e_peer = e + 1 - 2 * x
    c_y, c_k, c_ky = at.group(k, 1 - y), at.group(1 - k, y), at.group(1 - k, 1 - y)
    own_half = pl.ds(pl.multiple_of(x * half, LANES), half)
    peer_half = pl.ds(pl.multiple_of(ox * half, LANES), half)

    def chip(i):
        return lax.rem(z + i, chips)

    def route(to, w):
        return send(
            out_ref.at[2 * to + w], nv.at[c, w, e], route_s.at[to, w], route_r.at[z, w], (2 * to + x, k, y)
        )

    def route_in(s, w):
        ref = nv.at[c, w, 2 * s + x]
        return send(ref, ref, route_s.at[s, w], route_r.at[s, w], (2 * s + x, k, y))

    def x_hop(s, w, src):
        return send(src, nv.at[c, w, 2 * s + x], x_s.at[s, w], x_r.at[s, w], at.x_peer)

    def x_in(s, w):
        ref = nv.at[c, w, 2 * s + ox]
        return send(ref, ref, x_s.at[s, w], x_r.at[s, w], at.x_peer)

    def y_hop(s, w, src):
        return send(src, nv.at[c, w, s], y_s.at[s, w], y_r.at[s, w], at.y_peer)

    def y_in(s, w):
        ref = nv.at[c_y, w, s]
        return send(ref, ref, y_s.at[s, w], y_r.at[s, w], at.y_peer)

    def k_hop(v, s, w, src):
        return send(src, nv.at[at.group(k, v), w, s], d_s.at[v, s, w], d_r.at[v, s, w], at.k_peer)

    def k_in(v, s, w):
        ref = nv.at[at.group(1 - k, v), w, s]
        return send(ref, ref, d_s.at[v, s, w], d_r.at[v, s, w], at.k_peer)

    def eg_piece(i):
        part = pl.ds(pl.multiple_of(i * most, SUBLANES), most)
        return send(eg_ref.at[part, peer_half], eg_v.at[x, part], eg_s.at[i], eg_r.at[i], at.x_peer)

    def eg_in(i):
        ref = eg_v.at[ox, pl.ds(pl.multiple_of(i * most, SUBLANES), most)]
        return send(ref, ref, eg_s.at[i], eg_r.at[i], at.x_peer)

    eg_load = pltpu.make_async_copy(eg_ref.at[:, own_half], eg_v.at[x], local_sem.at[0])
    w_load = pltpu.make_async_copy(w_ref.at[:, own_half], wl, local_sem.at[1])
    w_keep = pltpu.make_async_copy(wl, wg_ref.at[e], local_sem.at[2])
    w_swap = send(w_ref.at[:, peer_half], wg_ref.at[e], w_x.at[0], w_x.at[1], at.x_peer)
    w_swap_in = send(wg_ref.at[e_peer], wg_ref.at[e_peer], w_x.at[0], w_x.at[1], at.x_peer)

    def w_hop(way, b, src=None):
        to = e + 2 if way == 0 else e - 2
        return send(
            wg_ref.at[b] if src is None else src, wg_ref.at[b], w_s.at[way, b], w_r.at[b],
            (2 * (to // 2) + x, k, y),
        )

    def w_own(b, src):
        for way in range(2):
            @pl.when(line.room(way, 0))
            def _():
                w_hop(way, b, src).start()

    def w_relay(distance, last):
        def one(way, b):
            w_hop(way, b).wait_recv()
            if not last:
                @pl.when(line.room(way, distance))
                def _():
                    w_hop(way, b).start()

        line.visit(distance, line.came, one)

    eg_load.start()
    w_load.start()
    at.greet()
    for w in range(2):
        loop(chips, lambda i: route(chip(i), w).start(), 1)
    w_swap.start()
    w_load.wait()
    w_own(e, wl)
    w_keep.start()

    def pass_on(s, w, src):
        x_hop(s, w, src).start()
        y_hop(2 * s + x, w, src).start()
        k_hop(y, 2 * s + x, w, src).start()

    for w in range(2):
        pass_on(z, w, out_ref.at[2 * z + w])
        eg_piece(w).start()
        nv[c, w, e] = out_ref[2 * z + w]

    def pass_route(i):
        s = chip(i)
        for w in range(2):
            route_in(s, w).wait_recv()
            pass_on(s, w, nv.at[c, w, 2 * s + x])
            eg_piece(2 * i + w).start()

    loop(chips, pass_route, 1)
    w_swap_in.wait_recv()
    w_own(e_peer, wg_ref.at[e_peer])

    def pass_x(i):
        s = chip(i)
        for w in range(2):
            x_in(s, w).wait_recv()
            ref = nv.at[c, w, 2 * s + ox]
            y_hop(2 * s + ox, w, ref).start()
            k_hop(y, 2 * s + ox, w, ref).start()

    loop(chips, pass_x)
    w_relay(1, groups == 3)

    def pass_y(parity):
        def one(i):
            s = 2 * chip(i) + parity
            for w in range(2):
                y_in(s, w).wait_recv()
                k_hop(1 - y, s, w, nv.at[c_y, w, s]).start()

        loop(chips, one)

    def wait_core(v):
        def one(s):
            for w in range(2):
                k_in(v, s, w).wait_recv()

        loop(senders, one)

    def product(group):
        total = None
        for w in range(2):
            term = lax.dot_general(
                nv[group, w].reshape(rows, width), eg_v[w], (((0,), (0,)), ((), ())), preferred_element_type=F32
            )
            total = term if total is None else total + term
        gw_ref[pl.ds(pl.multiple_of(group * width, SUBLANES), width), :] = total.astype(BF16)

    def keep(i, group):
        pltpu.make_async_copy(nv.at[group], n_ref.at[group], n_sem.at[i]).start()

    pass_y(x)
    eg_load.wait()
    loop(senders, lambda i: eg_in(i).wait_recv())
    eg_keep = pltpu.make_async_copy(eg_v, eg_out, local_sem.at[0])
    eg_keep.start()
    keep(0, c)
    product(c)
    wait_core(y)
    keep(1, c_k)
    product(c_k)
    pass_y(ox)
    keep(2, c_y)
    product(c_y)
    wait_core(1 - y)
    keep(3, c_ky)
    product(c_ky)
    for distance in range(2, groups - 1):
        w_relay(distance, distance == groups - 2)

    for distance in range(groups - 2):
        line.visit(distance, line.room, lambda way, b: w_hop(way, b).wait_send())
    w_swap.wait_send()
    w_keep.wait()
    for w in range(2):
        loop(chips, lambda i: route(chip(i), w).wait_send(), 1)

    def sent(s):
        eg_piece(s).wait_send()
        for w in range(2):
            y_hop(s, w, nv.at[c, w, s]).wait_send()
            for v in range(2):
                k_hop(v, s, w, nv.at[at.group(k, v), w, s]).wait_send()

    loop(senders, sent)
    for w in range(2):
        loop(chips, lambda s: x_hop(s, w, nv.at[c, w, 2 * s + x]).wait_send())
    eg_keep.wait()
    for i, group in enumerate((c, c_k, c_y, c_ky)):
        pltpu.make_async_copy(nv.at[group], n_ref.at[group], n_sem.at[i]).wait()


def spread(outgoing, embed_grad, proj_weight):
    senders, most, width = outgoing.shape
    chips = senders // 2
    groups = chips
    rows, cols = embed_grad.shape
    half = cols // 2
    dma = pltpu.SemaphoreType.DMA
    any_spec = pl.BlockSpec(memory_space=pl.ANY)
    vmem = pl.BlockSpec(memory_space=pltpu.VMEM)
    return pl.pallas_call(
        spread_kernel,
        out_shape=(
            jax.ShapeDtypeStruct((groups * width, half), BF16),
            jax.ShapeDtypeStruct((groups, 2, senders, most, width), BF16),
            jax.ShapeDtypeStruct((2, rows, half), BF16),
            jax.ShapeDtypeStruct((senders, proj_weight.shape[0], half), BF16),
        ),
        in_specs=[vmem, any_spec, any_spec],
        out_specs=(vmem, any_spec, any_spec, any_spec),
        scratch_shapes=[
            pltpu.VMEM((groups, 2, senders, most, width), BF16),
            pltpu.VMEM((2, rows, half), BF16),
            pltpu.VMEM((proj_weight.shape[0], half), BF16),
            dma((chips, 2)), dma((chips, 2)), dma((chips, 2)), dma((chips, 2)),
            dma((senders, 2)), dma((senders, 2)), dma((2, senders, 2)), dma((2, senders, 2)),
            dma((senders,)), dma((senders,)), dma((3,)), dma((groups,)), dma((2,)), dma((2, senders)), dma((senders,)),
        ],
        compiler_params=pltpu.CompilerParams(
            collective_id=0, has_side_effects=True, vmem_limit_bytes=56 * 1024 * 1024
        ),
        cost_estimate=pl.CostEstimate(
            flops=60 * 10**9, bytes_accessed=32 * rows * half, transcendentals=0
        ),
        name="spread",
    )(outgoing, embed_grad, proj_weight)


def finish_kernel(
    n_ref, wg_ref, eg_ref, g_ref, emb_ref, t_ref, sum_ref,
    rv, gs, g_load, r_s, r_r, q_s, q_keep,
    nv, wv, dv, ra, yb, xb, rb, ev, a_s, a_r, b_s, b_r, c_s, c_r, t_s, t_r, e_s, e_r, n_sem, l_sem, w_s, w_r, w_l,
):
    at = Place()
    line = Line(at)
    senders, most, width = t_ref.shape
    rows, half = eg_ref.shape[1:]
    groups = dv.shape[0]
    e, k, y, x, c, z = at.e, at.k, at.y, at.x, at.c, line.z
    ox, oy, ok = 1 - x, 1 - y, 1 - k
    c_y = at.group(k, oy)
    own_half = pl.ds(pl.multiple_of(x * half, LANES), half)
    peer_half = pl.ds(pl.multiple_of(ox * half, LANES), half)

    def turn(i):
        return lax.select(z < groups // 2, i, groups - 1 - i)

    last = turn(groups - 1)
    distant = (last - z == groups - 1) | (z - last == groups - 1)

    def load(w):
        return pltpu.make_async_copy(n_ref.at[:, w], nv, n_sem.at[0])

    def w_load(i):
        pair = pl.ds(2 * turn(i), 2)
        return pltpu.make_async_copy(wg_ref.at[pair], wv.at[pair], w_l.at[i])

    def w_hop(way, b):
        to = e + 2 if way == 0 else e - 2
        return send(wg_ref.at[b], wv.at[b], w_s.at[way, b], w_r.at[b], (2 * (to // 2) + x, k, y))

    for i in range(groups - 1):
        w_load(i).start()

    @pl.when(jnp.logical_not(distant))
    def _():
        w_load(groups - 1).start()

    load(ox).start()
    at.greet()
    line.visit(groups - 2, line.room, lambda way, b: w_hop(way, b).start())

    chips = g_ref.shape[0]
    piece_rows = g_ref.shape[2]
    tile = piece_rows // 5
    tiles = [pl.ds(i * tile, tile) for i in range(5)]

    def g_get(way, d, j):
        return pltpu.make_async_copy(g_ref.at[d, j], gs.at[way, j], g_load.at[way, j])

    def sum_hop(way, d, j, src):
        if way == 0:
            to, slot = e + 2, d
        else:
            to, slot = e - 2, lax.select(d == z - 1, chips, d)
        return send(
            src, rv.at[slot, j], r_s.at[way, d, j], r_r.at[way, d, j], (2 * (to // 2) + x, k, y)
        )

    def sum_in(way, d, j):
        return sum_hop(way, d, j, rv.at[d, j])

    def upstream(way):
        return z > 0 if way == 0 else z < chips - 1

    def downstream(way, d):
        return d > z if way == 0 else d < z

    def goal(way, i):
        return chips - 1 - i if way == 0 else i

    def over_j(fn):
        fn(ox)
        fn(x)

    for way in range(2):
        @pl.when(jnp.logical_not(upstream(way)))
        def _():
            for i in range(chips - 1):
                d = goal(way, i)
                over_j(lambda j: sum_hop(way, d, j, g_ref.at[d, j]).start())

    def relay(i, near):
        for way in range(2):
            d = goal(way, i)
            mine = (z < chips // 2) if (way == 0) == near else (z >= chips // 2)

            @pl.when(mine & upstream(way) & downstream(way, d))
            def _():
                over_j(lambda j: g_get(way, d, j).start())

                def one(j):
                    g_get(way, d, j).wait()
                    sum_in(way, d, j).wait_recv()
                    for t in tiles:
                        rv[d, j, t] = (rv[d, j, t].astype(F32) + gs[way, j, t].astype(F32)).astype(BF16)
                    sum_hop(way, d, j, rv.at[d, j]).start()

                over_j(one)

    def settle():
        def one(j):
            g_get(0, z, j).wait()
            for way in range(2):
                @pl.when(upstream(way))
                def _():
                    sum_in(way, z, j).wait_recv()

            def close(*slots):
                for t in tiles:
                    total = gs[0, j, t].astype(F32)
                    for slot in slots:
                        total = total + rv[slot, j, t].astype(F32)
                    rv[z, j, t] = total.astype(BF16)

            @pl.when(z == 0)
            def _():
                close(chips)

            @pl.when(z == chips - 1)
            def _():
                close(z)

            @pl.when((z > 0) & (z < chips - 1))
            def _():
                close(z, chips)

        over_j(lambda j: g_get(0, z, j).start())
        one(ox)
        swap.start()
        one(x)
        swap_keep.start()

    swap = send(rv.at[z, ox], sum_ref.at[:, own_half], q_s.at[0], q_s.at[1], at.x_peer)
    swap_in = send(sum_ref.at[:, peer_half], sum_ref.at[:, peer_half], q_s.at[0], q_s.at[1], at.x_peer)
    swap_keep = pltpu.make_async_copy(rv.at[z, x], sum_ref.at[:, own_half], q_keep.at[0])

    def sums_sent():
        for way in range(2):
            for i in range(chips - 1):
                d = goal(way, i)

                @pl.when(downstream(way, d))
                def _():
                    over_j(lambda j: sum_hop(way, d, j, rv.at[d, j]).wait_send())

    def weights(group):
        return wv[pl.ds(2 * group, 2)].reshape(width, half)

    def product(group):
        def one(w, carry):
            total = lax.dot_general(
                eg_ref[w], weights(group), (((1,), (1,)), ((), ())), preferred_element_type=F32
            )
            dv[group, w] = total.astype(BF16).reshape(senders, most, width)
            return carry

        lax.fori_loop(0, 2, one, 0)

    def core(v, s):
        return send(
            dv.at[at.group(ok, v), :, s], ra.at[v, :, s], a_s.at[v, s], a_r.at[v, s], at.k_peer
        )

    def across(s):
        return send(dv.at[c_y, :, s], yb.at[:, s], b_s.at[s], b_r.at[s], at.y_peer)

    def fold_core(s):
        core(oy, s).wait_recv()
        dv[c_y, :, s] = (dv[c_y, :, s].astype(F32) + ra[oy, :, s].astype(F32)).astype(BF16)
        across(s).start()

    def round_of(i):
        group = turn(i)
        product(group)

        @pl.when(group // 2 != k)
        def _():
            loop(senders, lambda s: core(group - 2 * (group // 2), s).start())

    def early(i):
        w_load(i).wait()
        round_of(i)

    for i in range(groups - 1):
        early(i)

    @pl.when(last != c_y)
    def _():
        loop(senders, fold_core)

    relay(0, True)

    @pl.when(jnp.logical_not(distant))
    def _():
        w_load(groups - 1).wait()

    line.visit(groups - 1, line.came, lambda way, b: w_hop(way, b).wait_recv())
    round_of(groups - 1)

    @pl.when(last == c_y)
    def _():
        loop(senders, fold_core)

    def embed(w):
        total = None
        for group in range(groups):
            term = jnp.dot(
                nv[group].reshape(rows, width), weights(group), preferred_element_type=F32
            )
            total = term if total is None else total + term
        ev[w] = total.astype(BF16)

    def part(s):
        return pl.ds(pl.multiple_of(s * most, SUBLANES), most)

    def emb_piece(s):
        return send(ev.at[ox, part(s)], emb_ref.at[part(s), own_half], e_s.at[s], e_r.at[s], at.x_peer)

    def emb_in(s):
        ref = emb_ref.at[part(s), peer_half]
        return send(ref, ref, e_s.at[s], e_r.at[s], at.x_peer)

    load(ox).wait()
    embed(ox)
    load(x).start()

    def to_x(s):
        return send(dv.at[c, ox, s], xb.at[s], c_s.at[s], c_r.at[s], at.x_peer)

    def fold_y(s):
        core(y, s).wait_recv()
        across(s).wait_recv()
        dv[c, :, s] = (
            dv[c, :, s].astype(F32) + ra[y, :, s].astype(F32) + yb[:, s].astype(F32)
        ).astype(BF16)
        to_x(s).start()
        emb_piece(s).start()

    def back(s):
        return send(rb.at[s], t_ref.at[e], t_s.at[s], t_r.at[e], (s, k, y))

    def fold_x(s):
        to_x(s).wait_recv()
        rb[s] = (dv[c, x, s].astype(F32) + xb[s].astype(F32)).astype(BF16)

        @pl.when(s == e)
        def _():
            t_ref[e] = rb[e]

        @pl.when(s != e)
        def _():
            back(s).start()

    fold_y(0)
    load(x).wait()
    embed(x)
    keep = pltpu.make_async_copy(ev.at[x], emb_ref.at[:, own_half], l_sem.at[0])
    keep.start()

    def step(s):
        fold_y(s)
        fold_x(s - 1)

    lax.fori_loop(1, senders // 2 - 1, lambda i, carry: (step(i), carry)[1], 0)
    for i in range(1, chips - 1):
        relay(i, True)
    for i in range(chips - 1):
        relay(i, False)
    lax.fori_loop(senders // 2 - 1, senders, lambda i, carry: (step(i), carry)[1], 0)
    fold_x(senders - 1)
    settle()

    def returned(i):
        s = at.other(i)
        send(rb.at[s], t_ref.at[s], t_s.at[s], t_r.at[s], (s, k, y)).wait_recv()
        back(s).wait_send()

    loop(senders, returned, 1)

    def sent(s):
        core(oy, s).wait_send()
        core(y, s).wait_send()
        across(s).wait_send()
        to_x(s).wait_send()
        emb_piece(s).wait_send()
        emb_in(s).wait_recv()

    loop(senders, sent)
    line.visit(groups - 2, line.room, lambda way, b: w_hop(way, b).wait_send())
    keep.wait()
    sums_sent()
    swap.wait_send()
    swap_in.wait_recv()
    swap_keep.wait()


def finish(shared, weight, grads, partial):
    groups, _, senders, most, width = shared.shape
    _, rows, half = grads.shape
    chips = partial.shape[0]
    dma = pltpu.SemaphoreType.DMA
    any_spec = pl.BlockSpec(memory_space=pl.ANY)
    vmem = pl.BlockSpec(memory_space=pltpu.VMEM)
    return pl.pallas_call(
        finish_kernel,
        out_shape=(
            jax.ShapeDtypeStruct((rows, 2 * half), BF16),
            jax.ShapeDtypeStruct((senders, most, width), BF16),
            jax.ShapeDtypeStruct((weight.shape[1], 2 * half), BF16),
        ),
        in_specs=[any_spec, any_spec, vmem, any_spec],
        out_specs=(any_spec, vmem, any_spec),
        scratch_shapes=[
            pltpu.VMEM((chips + 1, *partial.shape[1:]), BF16),
            pltpu.VMEM((2, *partial.shape[1:]), BF16),
            dma((2, 2)), dma((2, chips, 2)), dma((2, chips, 2)), dma((2,)), dma((1,)),
            pltpu.VMEM((groups, senders, most, width), BF16),
            pltpu.VMEM(weight.shape, BF16),
            pltpu.VMEM((groups, 2, senders, most, width), BF16),
            pltpu.VMEM((2, 2, senders, most, width), BF16),
            pltpu.VMEM((2, senders, most, width), BF16),
            pltpu.VMEM((senders, most, width), BF16),
            pltpu.VMEM((senders, most, width), BF16),
            pltpu.VMEM((2, rows, half), BF16),
            dma((2, senders)), dma((2, senders)), dma((senders,)), dma((senders,)),
            dma((senders,)), dma((senders,)), dma((senders,)), dma((senders,)),
            dma((senders,)), dma((senders,)), dma((1,)), dma((1,)),
            dma((2, senders)), dma((senders,)), dma((groups,)),
        ],
        compiler_params=pltpu.CompilerParams(
            collective_id=1, has_side_effects=True, vmem_limit_bytes=67043328
        ),
        cost_estimate=pl.CostEstimate(
            flops=60 * 10**9, bytes_accessed=32 * rows * half, transcendentals=0
        ),
        name="finish",
    )(shared, weight, grads, partial)


def row_kernel(mine, total, seen, send_sem, recv_sem):
    at = Place()
    groups = seen.shape[0]
    peers = [(k, y) for k in range(2) for y in range(2)]
    barrier = pltpu.get_barrier_semaphore()

    def others(fn):
        for k, y in peers:
            @pl.when(at.group(k, y) != at.c)
            def _():
                fn(k, y)

    others(
        lambda k, y: pl.semaphore_signal(barrier, inc=1, device_id=(at.e, k, y), device_id_type=MESH)
    )
    pl.semaphore_wait(barrier, groups - 1)

    def copy(k, y, slot):
        g = at.group(k, y)
        return send(mine, seen.at[slot], send_sem.at[g], recv_sem.at[slot], (at.e, k, y))

    others(lambda k, y: copy(k, y, at.c).start())
    seen[at.c] = mine[...]
    others(lambda k, y: copy(k, y, at.group(k, y)).wait_recv())
    result = seen[0]
    for g in range(1, groups):
        result = result + seen[g]
    total[...] = result
    others(lambda k, y: copy(k, y, at.c).wait_send())


def sum_rows(rows, groups):
    vmem = pl.BlockSpec(memory_space=pltpu.VMEM)
    return pl.pallas_call(
        row_kernel,
        out_shape=jax.ShapeDtypeStruct(rows.shape, F32),
        in_specs=[vmem],
        out_specs=vmem,
        scratch_shapes=[
            pltpu.VMEM((groups, *rows.shape), F32),
            pltpu.SemaphoreType.DMA((groups,)),
            pltpu.SemaphoreType.DMA((groups,)),
        ],
        compiler_params=pltpu.CompilerParams(collective_id=2, has_side_effects=True),
        name="sum_rows",
    )(rows)


def both_kernel(mine, mine_cols, total, total_cols, seen, seen_cols, r_s, r_r, c_s, c_r):
    at = Place()
    groups, senders = seen.shape[0], seen_cols.shape[0]
    peers = [(k, y) for k in range(2) for y in range(2)]
    barrier = pltpu.get_barrier_semaphore()

    def others(fn):
        for k, y in peers:
            @pl.when(at.group(k, y) != at.c)
            def _():
                fn(k, y)

    def along(fn):
        lax.fori_loop(1, senders, lambda i, carry: (fn(at.other(i)), carry)[1], 0)

    def signal(device):
        pl.semaphore_signal(barrier, inc=1, device_id=device, device_id_type=MESH)

    others(lambda k, y: signal((at.e, k, y)))
    along(lambda d: signal((d, at.k, at.y)))
    pl.semaphore_wait(barrier, groups + senders - 2)

    def copy(k, y, slot):
        g = at.group(k, y)
        return send(mine, seen.at[slot], r_s.at[g], r_r.at[slot], (at.e, k, y))

    def col(d, slot):
        return send(mine_cols, seen_cols.at[slot], c_s.at[d], c_r.at[slot], (d, at.k, at.y))

    others(lambda k, y: copy(k, y, at.c).start())
    along(lambda d: col(d, at.e).start())
    seen[at.c] = mine[...]
    seen_cols[at.e] = mine_cols[...]
    others(lambda k, y: copy(k, y, at.group(k, y)).wait_recv())
    along(lambda d: col(d, d).wait_recv())
    result = seen[0]
    for g in range(1, groups):
        result = result + seen[g]
    total[...] = result
    result = seen_cols[0]
    for d in range(1, senders):
        result = result + seen_cols[d]
    total_cols[...] = result
    others(lambda k, y: copy(k, y, at.c).wait_send())
    along(lambda d: col(d, at.e).wait_send())


def sum_both(rows, cols, groups, senders):
    vmem = pl.BlockSpec(memory_space=pltpu.VMEM)
    dma = pltpu.SemaphoreType.DMA
    return pl.pallas_call(
        both_kernel,
        out_shape=(
            jax.ShapeDtypeStruct(rows.shape, F32),
            jax.ShapeDtypeStruct(cols.shape, F32),
        ),
        in_specs=[vmem, vmem],
        out_specs=(vmem, vmem),
        scratch_shapes=[
            pltpu.VMEM((groups, *rows.shape), F32),
            pltpu.VMEM((senders, *cols.shape), F32),
            dma((groups,)), dma((groups,)), dma((senders,)), dma((senders,)),
        ],
        compiler_params=pltpu.CompilerParams(collective_id=3, has_side_effects=True),
        name="sum_both",
    )(rows, cols)


def owner_body(patches, gain, shift, proj_weight, llm_rank, embed_grad):
    features = ("section", "llmdp")
    own_rows, owned_width = patches.shape
    width = gain.shape[0]
    senders = lax.axis_size("enc")
    most_slots = embed_grad.shape[0] // senders
    groups = width // owned_width
    column_start = lax.axis_index(features) * owned_width
    gain_own = lax.dynamic_slice_in_dim(gain, column_start, owned_width, 0)
    shift_own = lax.dynamic_slice_in_dim(shift, column_start, owned_width, 0)
    values = patches.astype(F32)
    total, squares = sum_rows(jnp.stack([jnp.sum(values, 1), jnp.sum(values * values, 1)]), groups)
    average = (total / width)[:, None]
    variance = (squares / width)[:, None] - average * average
    deviation = lax.rsqrt(variance + EPSILON)
    standardized = (values - average) * deviation
    normed = (standardized * gain_own + shift_own).astype(BF16)

    slot = slots_of(llm_rank, senders, most_slots)
    places = jnp.arange(senders * most_slots, dtype=jnp.int32)
    chosen = (places[:, None] == slot[None, :]).astype(BF16)
    outgoing = jnp.dot(chosen, normed, preferred_element_type=F32).astype(BF16)
    grad_partial, shared, grads, weight = spread(
        outgoing.reshape(senders, most_slots, owned_width), embed_grad, proj_weight
    )
    embeds_recv, returned, grad_sum = finish(
        shared, weight, grads,
        grad_partial.reshape(senders // 2, 2, weight.shape[1], weight.shape[2]),
    )
    grad_weight = grad_sum.astype(F32)
    dnormed = lax.dot_general(
        chosen, returned.reshape(senders * most_slots, owned_width), (((0,), (0,)), ((), ())),
        preferred_element_type=F32,
    )
    dxhat = dnormed * gain_own
    (mean_sum, cross_sum), (gain_gradient, grad_shift) = sum_both(
        jnp.stack([jnp.sum(dxhat, 1), jnp.sum(dxhat * standardized, 1)]),
        jnp.stack([jnp.sum(dnormed * standardized, 0), jnp.sum(dnormed, 0)]),
        groups,
        senders,
    )
    hidden_state_gradient = (
        deviation
        * (dxhat - (mean_sum / width)[:, None] - standardized * (cross_sum / width)[:, None])
    ).astype(BF16)
    return (embeds_recv, hidden_state_gradient, grad_weight, gain_gradient, grad_shift)


def plain_body(patches, gain, shift, proj_weight, llm_rank, embed_grad):
    features = ("section", "llmdp")
    own_rows, owned_width = patches.shape
    width = gain.shape[0]
    weight_rows, out_cols = proj_weight.shape
    senders = lax.axis_size("enc")
    block = block_size(senders, out_cols)
    near = [[b * block + i for i in range(block)] for b in range(senders // block)]
    far = [[b * block + i for b in range(senders // block)] for i in range(block)]

    def near_exchange(x, split, concat):
        return lax.all_to_all(x, "enc", split, concat, axis_index_groups=near, tiled=True)

    column_start = lax.axis_index(features) * owned_width
    gain_own = lax.dynamic_slice_in_dim(gain, column_start, owned_width, 0)

    weight_part = near_exchange(proj_weight, 1, 0)
    weight = lax.all_gather(weight_part, "enc", axis=0, axis_index_groups=far, tiled=True)

    block_rows = lax.all_gather(patches, "enc", axis=0, axis_index_groups=near, tiled=True)
    complete_rows = lax.all_gather(block_rows, features, axis=1, tiled=True).astype(jnp.float32)
    row_average = jnp.mean(complete_rows, 1, keepdims=True)
    variance = jnp.mean(complete_rows * complete_rows, 1, keepdims=True) - row_average * row_average
    inverse_deviation = lax.rsqrt(variance + EPSILON)
    standardized = (complete_rows - row_average) * inverse_deviation
    normed = (standardized * gain + shift).astype(jnp.bfloat16)

    row_start = (lax.axis_index("enc") % block) * own_rows
    average_own = lax.dynamic_slice_in_dim(row_average, row_start, own_rows, 0)
    deviation_own = lax.dynamic_slice_in_dim(inverse_deviation, row_start, own_rows, 0)
    standardized_owned = (patches.astype(jnp.float32) - average_own) * deviation_own

    most_slots = embed_grad.shape[0] // senders
    target = llm_rank[:, 0]
    owners = jnp.arange(senders, dtype=jnp.int32)
    hits = (target[:, None] == owners[None, :]).astype(jnp.int32)
    rank = jnp.sum((jnp.cumsum(hits, 0) - hits) * hits, 1)
    slot = target * most_slots + rank

    def enc_exchange(x):
        return lax.all_to_all(
            x.reshape(senders, most_slots, out_cols), "enc", split_axis=0, concat_axis=0, tiled=True
        ).reshape(senders * most_slots, out_cols)

    d_embed = near_exchange(enc_exchange(embed_grad)[slot], 1, 0)
    grad_part = lax.psum_scatter(
        lax.dot_general(
            normed, d_embed, (((0,), (0,)), ((), ())), preferred_element_type=jnp.float32
        ).astype(jnp.bfloat16),
        "enc",
        scatter_dimension=0,
        axis_index_groups=far,
        tiled=True,
    )
    grad_weight = near_exchange(grad_part, 0, 1).astype(jnp.float32)

    embed_part = jnp.dot(normed, weight, preferred_element_type=jnp.float32).astype(jnp.bfloat16)
    embed = near_exchange(embed_part, 0, 1)
    outgoing = jnp.zeros((senders * most_slots, out_cols), jnp.bfloat16).at[slot].set(embed)
    embeds_recv = enc_exchange(outgoing)

    partial_grad = lax.dot_general(
        d_embed, weight, (((1,), (1,)), ((), ())), preferred_element_type=jnp.float32
    )
    group_count = width // owned_width
    pieces = partial_grad.astype(jnp.bfloat16).reshape(block * own_rows, group_count, owned_width)
    columns = lax.all_to_all(pieces, features, split_axis=1, concat_axis=1, tiled=True)
    column_sum = jnp.sum(columns.astype(jnp.float32), 1).astype(jnp.bfloat16)
    shares = near_exchange(column_sum.reshape(block, own_rows, owned_width), 0, 0)
    owned_normalized_gradient = jnp.sum(shares.astype(jnp.float32), 0)
    owned_centered_gradient = owned_normalized_gradient * gain_own
    mean_sum, cross_sum = lax.psum(
        (
            jnp.sum(owned_centered_gradient, 1),
            jnp.sum(owned_centered_gradient * standardized_owned, 1),
        ),
        features,
    )
    gradient_row_average = (mean_sum / width)[:, None]
    gradient_cross_product = (cross_sum / width)[:, None]
    hidden_state_gradient = (
        deviation_own
        * (
            owned_centered_gradient
            - gradient_row_average
            - standardized_owned * gradient_cross_product
        )
    ).astype(jnp.bfloat16)
    gain_gradient, grad_shift = lax.psum(
        (
            jnp.sum(owned_normalized_gradient * standardized_owned, 0),
            jnp.sum(owned_normalized_gradient, 0),
        ),
        "enc",
    )
    return (embeds_recv, hidden_state_gradient, grad_weight, gain_gradient, grad_shift)


def fits(patches, gain, proj_weight, embed_grad):
    senders, cores, rows_of = (lax.axis_size(a) for a in ("enc", "section", "llmdp"))
    most = embed_grad.shape[0] // senders
    return (
        cores == 2
        and rows_of == 2
        and block_size(senders, proj_weight.shape[1]) == 2
        and senders // 2 == cores * rows_of
        and most % SUBLANES == 0
        and proj_weight.shape[0] % SUBLANES == 0
        and patches.shape[1] == 2 * proj_weight.shape[0]
    )


def body(patches, gain, shift, proj_weight, llm_rank, embed_grad):
    form = owner_body if fits(patches, gain, proj_weight, embed_grad) else plain_body
    return form(patches, gain, shift, proj_weight, llm_rank, embed_grad)


def solution(mesh):
    in_specs = (
        P("enc", ("section", "llmdp")),
        P(),
        P(),
        P("enc", ("section", "llmdp")),
        P("enc", None),
        P("enc", ("section", "llmdp")),
    )
    out_specs = (
        P("enc", ("section", "llmdp")),
        P("enc", ("section", "llmdp")),
        P("enc", ("section", "llmdp")),
        P(("section", "llmdp")),
        P(("section", "llmdp")),
    )
    return jax.shard_map(body, mesh=mesh, in_specs=in_specs, out_specs=out_specs, check_vma=False)
```

```python
import functools

import jax
import jax.numpy as jnp
from jax import lax
from jax.experimental import pallas as pl
from jax.experimental.pallas import tpu as pltpu
from jax.sharding import PartitionSpec as P

EPSILON = 1e-05
MESH = pl.DeviceIdType.MESH
F32 = jnp.float32
BF16 = jnp.bfloat16

MAX_BLOCK = 2
SUBLANES = 16
LANES = 128


def block_size(senders, out_cols):
    size = MAX_BLOCK
    while size > 1 and (senders % size or senders == size or out_cols % (size * 128)):
        size //= 2
    return size


def slots_of(llm_rank, senders, most_slots):
    target = llm_rank[:, 0]
    owners = jnp.arange(senders, dtype=jnp.int32)
    hits = (target[:, None] == owners[None, :]).astype(jnp.int32)
    rank = jnp.sum((jnp.cumsum(hits, 0) - hits) * hits, 1)
    return target * most_slots + rank


class Place:
    def __init__(self):
        self.e = lax.axis_index("enc")
        self.k = lax.axis_index("section")
        self.y = lax.axis_index("llmdp")
        self.x = lax.rem(self.e, 2)
        self.senders = lax.axis_size("enc")
        self.c = self.group(self.k, self.y)
        self.x_peer = (self.e + 1 - 2 * self.x, self.k, self.y)
        self.y_peer = (self.e, self.k, 1 - self.y)
        self.k_peer = (self.e, 1 - self.k, self.y)

    def group(self, k, y):
        return k * 2 + y

    def other(self, step):
        return lax.rem(self.e + step, self.senders)

    def greet(self):
        barrier = pltpu.get_barrier_semaphore()

        def one(step, carry):
            pl.semaphore_signal(
                barrier, inc=1, device_id=(self.other(step), self.k, self.y), device_id_type=MESH
            )
            return carry

        lax.fori_loop(1, self.senders, one, 0)
        for peer in (self.y_peer, self.k_peer):
            pl.semaphore_signal(barrier, inc=1, device_id=peer, device_id_type=MESH)
        pl.semaphore_wait(barrier, self.senders + 1)


def send(src, dst, send_sem, recv_sem, device):
    return pltpu.make_async_remote_copy(
        src_ref=src, dst_ref=dst, send_sem=send_sem, recv_sem=recv_sem, device_id=device, device_id_type=MESH
    )


def loop(count, fn, start=0):
    lax.fori_loop(start, count, lambda i, carry: (fn(i), carry)[1], 0)


class Line:
    def __init__(self, at):
        self.z = at.e // 2
        self.count = at.senders // 2
        self.parities = (at.x, 1 - at.x)

    def came(self, way, distance):
        return self.z >= distance if way == 0 else self.z + distance < self.count

    def room(self, way, distance):
        if way == 0:
            return (self.z >= distance) & (self.z + 1 < self.count)
        return (self.z + distance < self.count) & (self.z >= 1)

    def block(self, way, distance, parity):
        return 2 * (self.z - distance if way == 0 else self.z + distance) + parity

    def visit(self, distance, condition, fn, parities=None):
        for parity in self.parities if parities is None else parities:
            for way in range(2):
                @pl.when(condition(way, distance))
                def _():
                    fn(way, self.block(way, distance, parity))


def spread_kernel(
    out_ref, eg_ref, w_ref, gw_ref, n_ref, eg_out, wg_ref,
    nv, eg_v, wl, acc, route_s, route_r, x_s, x_r, y_s, y_r, d_s, d_r, eg_s, eg_r, local_sem, n_sem, w_x, w_s, w_r,
):
    at = Place()
    line = Line(at)
    senders, most, width = out_ref.shape
    rows, half = eg_v.shape[1:]
    groups = nv.shape[0]
    chips = senders // 2
    e, k, y, x, c, z = at.e, at.k, at.y, at.x, at.c, line.z
    ox = 1 - x
    e_peer = e + 1 - 2 * x
    c_y, c_k, c_ky = at.group(k, 1 - y), at.group(1 - k, y), at.group(1 - k, 1 - y)
    own_half = pl.ds(pl.multiple_of(x * half, LANES), half)
    peer_half = pl.ds(pl.multiple_of(ox * half, LANES), half)

    def chip(i):
        return lax.rem(z + i, chips)

    def route(to, w):
        return send(
            out_ref.at[2 * to + w], nv.at[c, w, e], route_s.at[to, w], route_r.at[z, w], (2 * to + x, k, y)
        )

    def route_in(s, w):
        ref = nv.at[c, w, 2 * s + x]
        return send(ref, ref, route_s.at[s, w], route_r.at[s, w], (2 * s + x, k, y))

    def x_hop(s, w, src):
        return send(src, nv.at[c, w, 2 * s + x], x_s.at[s, w], x_r.at[s, w], at.x_peer)

    def x_in(s, w):
        ref = nv.at[c, w, 2 * s + ox]
        return send(ref, ref, x_s.at[s, w], x_r.at[s, w], at.x_peer)

    def y_hop(s, w, src):
        return send(src, nv.at[c, w, s], y_s.at[s, w], y_r.at[s, w], at.y_peer)

    def y_in(s, w):
        ref = nv.at[c_y, w, s]
        return send(ref, ref, y_s.at[s, w], y_r.at[s, w], at.y_peer)

    def k_hop(v, s, w, src):
        return send(src, nv.at[at.group(k, v), w, s], d_s.at[v, s, w], d_r.at[v, s, w], at.k_peer)

    def k_in(v, s, w):
        ref = nv.at[at.group(1 - k, v), w, s]
        return send(ref, ref, d_s.at[v, s, w], d_r.at[v, s, w], at.k_peer)

    def eg_piece(i):
        part = pl.ds(pl.multiple_of(i * most, SUBLANES), most)
        return send(eg_ref.at[part, peer_half], eg_v.at[x, part], eg_s.at[i], eg_r.at[i], at.x_peer)

    def eg_in(i):
        ref = eg_v.at[ox, pl.ds(pl.multiple_of(i * most, SUBLANES), most)]
        return send(ref, ref, eg_s.at[i], eg_r.at[i], at.x_peer)

    eg_load = pltpu.make_async_copy(eg_ref.at[:, own_half], eg_v.at[x], local_sem.at[0])
    w_load = pltpu.make_async_copy(w_ref.at[:, own_half], wl, local_sem.at[1])
    w_keep = pltpu.make_async_copy(wl, wg_ref.at[e], local_sem.at[2])
    w_swap = send(w_ref.at[:, peer_half], wg_ref.at[e], w_x.at[0], w_x.at[1], at.x_peer)
    w_swap_in = send(wg_ref.at[e_peer], wg_ref.at[e_peer], w_x.at[0], w_x.at[1], at.x_peer)

    def w_hop(way, b, src=None):
        to = e + 2 if way == 0 else e - 2
        return send(
            wg_ref.at[b] if src is None else src, wg_ref.at[b], w_s.at[way, b], w_r.at[b],
            (2 * (to // 2) + x, k, y),
        )

    def w_own(b, src):
        for way in range(2):
            @pl.when(line.room(way, 0))
            def _():
                w_hop(way, b, src).start()

    def w_relay(distance, last, parities=None):
        def one(way, b):
            w_hop(way, b).wait_recv()
            if not last:
                @pl.when(line.room(way, distance))
                def _():
                    w_hop(way, b).start()

        line.visit(distance, line.came, one, parities)

    eg_load.start()
    w_load.start()
    at.greet()
    for w in range(2):
        loop(chips, lambda i: route(chip(i), w).start(), 1)
    w_swap.start()
    w_load.wait()
    w_own(e, wl)
    w_keep.start()

    def pass_on(s, w, src):
        x_hop(s, w, src).start()
        y_hop(2 * s + x, w, src).start()
        k_hop(y, 2 * s + x, w, src).start()

    for w in range(2):
        pass_on(z, w, out_ref.at[2 * z + w])
        nv[c, w, e] = out_ref[2 * z + w]

    def pass_route(i):
        s = chip(i)
        for w in range(2):
            route_in(s, w).wait_recv()
            pass_on(s, w, nv.at[c, w, 2 * s + x])

    loop(chips, pass_route, 1)
    loop(senders, lambda i: eg_piece(i).start())
    w_swap_in.wait_recv()
    w_own(e_peer, wg_ref.at[e_peer])
    w_relay(1, groups == 3, (x,))

    def pass_x(i):
        s = chip(i)
        for w in range(2):
            x_in(s, w).wait_recv()
            ref = nv.at[c, w, 2 * s + ox]
            y_hop(2 * s + ox, w, ref).start()
            k_hop(y, 2 * s + ox, w, ref).start()

    loop(chips, pass_x)
    w_relay(1, groups == 3, (ox,))

    def pass_y(parity):
        def one(i):
            s = 2 * chip(i) + parity
            for w in range(2):
                y_in(s, w).wait_recv()
                k_hop(1 - y, s, w, nv.at[c_y, w, s]).start()

        loop(chips, one)

    def wait_core(v):
        def one(s):
            for w in range(2):
                k_in(v, s, w).wait_recv()

        loop(senders, one)

    def term(group, w):
        return lax.dot_general(
            nv[group, w].reshape(rows, width), eg_v[w], (((0,), (0,)), ((), ())), preferred_element_type=F32
        )

    def own_term(i, group):
        acc[i] = term(group, x)

    def peer_term(i, group):
        gw_ref[pl.ds(pl.multiple_of(group * width, SUBLANES), width), :] = (
            acc[i] + term(group, ox)
        ).astype(BF16)

    def keep(i, group):
        pltpu.make_async_copy(nv.at[group], n_ref.at[group], n_sem.at[i]).start()

    eg_load.wait()
    pass_y(x)
    keep(0, c)
    own_term(0, c)
    wait_core(y)
    keep(1, c_k)
    own_term(1, c_k)
    pass_y(ox)
    keep(2, c_y)
    own_term(2, c_y)
    loop(senders, lambda i: eg_in(i).wait_recv())
    eg_keep = pltpu.make_async_copy(eg_v, eg_out, local_sem.at[0])
    eg_keep.start()
    peer_term(0, c)
    peer_term(1, c_k)
    wait_core(1 - y)
    keep(3, c_ky)
    own_term(3, c_ky)
    peer_term(2, c_y)
    peer_term(3, c_ky)
    for distance in range(2, groups - 1):
        w_relay(distance, distance == groups - 2)

    for distance in range(groups - 2):
        line.visit(distance, line.room, lambda way, b: w_hop(way, b).wait_send())
    w_swap.wait_send()
    w_keep.wait()
    for w in range(2):
        loop(chips, lambda i: route(chip(i), w).wait_send(), 1)

    def sent(s):
        eg_piece(s).wait_send()
        for w in range(2):
            y_hop(s, w, nv.at[c, w, s]).wait_send()
            for v in range(2):
                k_hop(v, s, w, nv.at[at.group(k, v), w, s]).wait_send()

    loop(senders, sent)
    for w in range(2):
        loop(chips, lambda s: x_hop(s, w, nv.at[c, w, 2 * s + x]).wait_send())
    eg_keep.wait()
    for i, group in enumerate((c, c_k, c_y, c_ky)):
        pltpu.make_async_copy(nv.at[group], n_ref.at[group], n_sem.at[i]).wait()


def spread(outgoing, embed_grad, proj_weight):
    senders, most, width = outgoing.shape
    chips = senders // 2
    groups = chips
    rows, cols = embed_grad.shape
    half = cols // 2
    dma = pltpu.SemaphoreType.DMA
    any_spec = pl.BlockSpec(memory_space=pl.ANY)
    vmem = pl.BlockSpec(memory_space=pltpu.VMEM)
    return pl.pallas_call(
        spread_kernel,
        out_shape=(
            jax.ShapeDtypeStruct((groups * width, half), BF16),
            jax.ShapeDtypeStruct((groups, 2, senders, most, width), BF16),
            jax.ShapeDtypeStruct((2, rows, half), BF16),
            jax.ShapeDtypeStruct((senders, proj_weight.shape[0], half), BF16),
        ),
        in_specs=[vmem, any_spec, any_spec],
        out_specs=(vmem, any_spec, any_spec, any_spec),
        scratch_shapes=[
            pltpu.VMEM((groups, 2, senders, most, width), BF16),
            pltpu.VMEM((2, rows, half), BF16),
            pltpu.VMEM((proj_weight.shape[0], half), BF16),
            pltpu.VMEM((groups, width, half), F32),
            dma((chips, 2)), dma((chips, 2)), dma((chips, 2)), dma((chips, 2)),
            dma((senders, 2)), dma((senders, 2)), dma((2, senders, 2)), dma((2, senders, 2)),
            dma((senders,)), dma((senders,)), dma((3,)), dma((groups,)), dma((2,)), dma((2, senders)), dma((senders,)),
        ],
        compiler_params=pltpu.CompilerParams(
            collective_id=0, has_side_effects=True, vmem_limit_bytes=56 * 1024 * 1024
        ),
        cost_estimate=pl.CostEstimate(
            flops=60 * 10**9, bytes_accessed=32 * rows * half, transcendentals=0
        ),
        name="spread",
    )(outgoing, embed_grad, proj_weight)


def finish_kernel(
    n_ref, wg_ref, eg_ref, g_ref, emb_ref, t_ref, sum_ref,
    rv, gs, g_load, r_s, r_r, q_s, q_keep,
    nv, wv, dv, ra, yb, xb, rb, ev, a_s, a_r, b_s, b_r, c_s, c_r, t_s, t_r, e_s, e_r, n_sem, l_sem, w_s, w_r, w_l,
):
    at = Place()
    line = Line(at)
    senders, most, width = t_ref.shape
    rows, half = eg_ref.shape[1:]
    groups = dv.shape[0]
    e, k, y, x, c, z = at.e, at.k, at.y, at.x, at.c, line.z
    ox, oy, ok = 1 - x, 1 - y, 1 - k
    c_y = at.group(k, oy)
    own_half = pl.ds(pl.multiple_of(x * half, LANES), half)
    peer_half = pl.ds(pl.multiple_of(ox * half, LANES), half)

    def turn(i):
        return lax.select(z < groups // 2, i, groups - 1 - i)

    last = turn(groups - 1)
    distant = (last - z == groups - 1) | (z - last == groups - 1)

    def load(w):
        return pltpu.make_async_copy(n_ref.at[:, w], nv, n_sem.at[0])

    def w_load(i):
        pair = pl.ds(2 * turn(i), 2)
        return pltpu.make_async_copy(wg_ref.at[pair], wv.at[pair], w_l.at[i])

    def w_hop(way, b):
        to = e + 2 if way == 0 else e - 2
        return send(wg_ref.at[b], wv.at[b], w_s.at[way, b], w_r.at[b], (2 * (to // 2) + x, k, y))

    for i in range(groups - 1):
        w_load(i).start()

    @pl.when(jnp.logical_not(distant))
    def _():
        w_load(groups - 1).start()

    load(ox).start()
    at.greet()
    line.visit(groups - 2, line.room, lambda way, b: w_hop(way, b).start())

    chips = g_ref.shape[0]
    piece_rows = g_ref.shape[2]
    tile = piece_rows // 5
    tiles = [pl.ds(i * tile, tile) for i in range(5)]

    def g_get(way, d, j):
        return pltpu.make_async_copy(g_ref.at[d, j], gs.at[way, j], g_load.at[way, j])

    def sum_hop(way, d, j, src):
        if way == 0:
            to, slot = e + 2, d
        else:
            to, slot = e - 2, lax.select(d == z - 1, chips, d)
        return send(
            src, rv.at[slot, j], r_s.at[way, d, j], r_r.at[way, d, j], (2 * (to // 2) + x, k, y)
        )

    def sum_in(way, d, j):
        return sum_hop(way, d, j, rv.at[d, j])

    def upstream(way):
        return z > 0 if way == 0 else z < chips - 1

    def downstream(way, d):
        return d > z if way == 0 else d < z

    def goal(way, i):
        return chips - 1 - i if way == 0 else i

    def over_j(fn):
        fn(ox)
        fn(x)

    for way in range(2):
        @pl.when(jnp.logical_not(upstream(way)))
        def _():
            for i in range(chips - 1):
                d = goal(way, i)
                over_j(lambda j: sum_hop(way, d, j, g_ref.at[d, j]).start())

    def relay(i, near):
        for way in range(2):
            d = goal(way, i)
            mine = (z < chips // 2) if (way == 0) == near else (z >= chips // 2)

            @pl.when(mine & upstream(way) & downstream(way, d))
            def _():
                over_j(lambda j: g_get(way, d, j).start())

                def one(j):
                    g_get(way, d, j).wait()
                    sum_in(way, d, j).wait_recv()
                    for t in tiles:
                        rv[d, j, t] = (rv[d, j, t].astype(F32) + gs[way, j, t].astype(F32)).astype(BF16)
                    sum_hop(way, d, j, rv.at[d, j]).start()

                over_j(one)

    def settle():
        def one(j):
            g_get(0, z, j).wait()
            for way in range(2):
                @pl.when(upstream(way))
                def _():
                    sum_in(way, z, j).wait_recv()

            def close(*slots):
                for t in tiles:
                    total = gs[0, j, t].astype(F32)
                    for slot in slots:
                        total = total + rv[slot, j, t].astype(F32)
                    rv[z, j, t] = total.astype(BF16)

            @pl.when(z == 0)
            def _():
                close(chips)

            @pl.when(z == chips - 1)
            def _():
                close(z)

            @pl.when((z > 0) & (z < chips - 1))
            def _():
                close(z, chips)

        over_j(lambda j: g_get(0, z, j).start())
        one(ox)
        swap.start()
        one(x)
        swap_keep.start()

    swap = send(rv.at[z, ox], sum_ref.at[:, own_half], q_s.at[0], q_s.at[1], at.x_peer)
    swap_in = send(sum_ref.at[:, peer_half], sum_ref.at[:, peer_half], q_s.at[0], q_s.at[1], at.x_peer)
    swap_keep = pltpu.make_async_copy(rv.at[z, x], sum_ref.at[:, own_half], q_keep.at[0])

    def sums_sent():
        for way in range(2):
            for i in range(chips - 1):
                d = goal(way, i)

                @pl.when(downstream(way, d))
                def _():
                    over_j(lambda j: sum_hop(way, d, j, rv.at[d, j]).wait_send())

    def weights(group):
        return wv[pl.ds(2 * group, 2)].reshape(width, half)

    def product(group):
        def one(w, carry):
            total = lax.dot_general(
                eg_ref[w], weights(group), (((1,), (1,)), ((), ())), preferred_element_type=F32
            )
            dv[group, w] = total.astype(BF16).reshape(senders, most, width)
            return carry

        lax.fori_loop(0, 2, one, 0)

    def core(v, s):
        return send(
            dv.at[at.group(ok, v), :, s], ra.at[v, :, s], a_s.at[v, s], a_r.at[v, s], at.k_peer
        )

    def across(s):
        return send(dv.at[c_y, :, s], yb.at[:, s], b_s.at[s], b_r.at[s], at.y_peer)

    def fold_core(s):
        core(oy, s).wait_recv()
        dv[c_y, :, s] = (dv[c_y, :, s].astype(F32) + ra[oy, :, s].astype(F32)).astype(BF16)
        across(s).start()

    def round_of(i):
        group = turn(i)
        product(group)

        @pl.when(group // 2 != k)
        def _():
            loop(senders, lambda s: core(group - 2 * (group // 2), s).start())

    def early(i):
        w_load(i).wait()
        round_of(i)

    for i in range(groups - 1):
        early(i)

    @pl.when(last != c_y)
    def _():
        loop(senders, fold_core)

    relay(0, True)

    @pl.when(jnp.logical_not(distant))
    def _():
        w_load(groups - 1).wait()

    line.visit(groups - 1, line.came, lambda way, b: w_hop(way, b).wait_recv())
    round_of(groups - 1)

    @pl.when(last == c_y)
    def _():
        loop(senders, fold_core)

    def embed(w):
        total = None
        for group in range(groups):
            term = jnp.dot(
                nv[group].reshape(rows, width), weights(group), preferred_element_type=F32
            )
            total = term if total is None else total + term
        ev[w] = total.astype(BF16)

    def part(s):
        return pl.ds(pl.multiple_of(s * most, SUBLANES), most)

    def emb_piece(s):
        return send(ev.at[ox, part(s)], emb_ref.at[part(s), own_half], e_s.at[s], e_r.at[s], at.x_peer)

    def emb_in(s):
        ref = emb_ref.at[part(s), peer_half]
        return send(ref, ref, e_s.at[s], e_r.at[s], at.x_peer)

    load(ox).wait()
    embed(ox)
    load(x).start()

    def to_x(s):
        return send(dv.at[c, ox, s], xb.at[s], c_s.at[s], c_r.at[s], at.x_peer)

    def fold_y(s):
        core(y, s).wait_recv()
        across(s).wait_recv()
        dv[c, :, s] = (
            dv[c, :, s].astype(F32) + ra[y, :, s].astype(F32) + yb[:, s].astype(F32)
        ).astype(BF16)
        to_x(s).start()
        emb_piece(s).start()

    def back(s):
        return send(rb.at[s], t_ref.at[e], t_s.at[s], t_r.at[e], (s, k, y))

    def fold_x(s):
        to_x(s).wait_recv()
        rb[s] = (dv[c, x, s].astype(F32) + xb[s].astype(F32)).astype(BF16)

        @pl.when(s == e)
        def _():
            t_ref[e] = rb[e]

        @pl.when(s != e)
        def _():
            back(s).start()

    fold_y(0)
    load(x).wait()
    embed(x)
    keep = pltpu.make_async_copy(ev.at[x], emb_ref.at[:, own_half], l_sem.at[0])
    keep.start()

    def step(s):
        fold_y(s)
        fold_x(s - 1)

    lax.fori_loop(1, senders // 2 - 1, lambda i, carry: (step(i), carry)[1], 0)
    for i in range(1, chips - 1):
        relay(i, True)
    for i in range(chips - 1):
        relay(i, False)
    lax.fori_loop(senders // 2 - 1, senders, lambda i, carry: (step(i), carry)[1], 0)
    fold_x(senders - 1)
    settle()

    def returned(i):
        s = at.other(i)
        send(rb.at[s], t_ref.at[s], t_s.at[s], t_r.at[s], (s, k, y)).wait_recv()
        back(s).wait_send()

    loop(senders, returned, 1)

    def sent(s):
        core(oy, s).wait_send()
        core(y, s).wait_send()
        across(s).wait_send()
        to_x(s).wait_send()
        emb_piece(s).wait_send()
        emb_in(s).wait_recv()

    loop(senders, sent)
    line.visit(groups - 2, line.room, lambda way, b: w_hop(way, b).wait_send())
    keep.wait()
    sums_sent()
    swap.wait_send()
    swap_in.wait_recv()
    swap_keep.wait()


def finish(shared, weight, grads, partial):
    groups, _, senders, most, width = shared.shape
    _, rows, half = grads.shape
    chips = partial.shape[0]
    dma = pltpu.SemaphoreType.DMA
    any_spec = pl.BlockSpec(memory_space=pl.ANY)
    vmem = pl.BlockSpec(memory_space=pltpu.VMEM)
    return pl.pallas_call(
        finish_kernel,
        out_shape=(
            jax.ShapeDtypeStruct((rows, 2 * half), BF16),
            jax.ShapeDtypeStruct((senders, most, width), BF16),
            jax.ShapeDtypeStruct((weight.shape[1], 2 * half), BF16),
        ),
        in_specs=[any_spec, any_spec, vmem, any_spec],
        out_specs=(any_spec, vmem, any_spec),
        scratch_shapes=[
            pltpu.VMEM((chips + 1, *partial.shape[1:]), BF16),
            pltpu.VMEM((2, *partial.shape[1:]), BF16),
            dma((2, 2)), dma((2, chips, 2)), dma((2, chips, 2)), dma((2,)), dma((1,)),
            pltpu.VMEM((groups, senders, most, width), BF16),
            pltpu.VMEM(weight.shape, BF16),
            pltpu.VMEM((groups, 2, senders, most, width), BF16),
            pltpu.VMEM((2, 2, senders, most, width), BF16),
            pltpu.VMEM((2, senders, most, width), BF16),
            pltpu.VMEM((senders, most, width), BF16),
            pltpu.VMEM((senders, most, width), BF16),
            pltpu.VMEM((2, rows, half), BF16),
            dma((2, senders)), dma((2, senders)), dma((senders,)), dma((senders,)),
            dma((senders,)), dma((senders,)), dma((senders,)), dma((senders,)),
            dma((senders,)), dma((senders,)), dma((1,)), dma((1,)),
            dma((2, senders)), dma((senders,)), dma((groups,)),
        ],
        compiler_params=pltpu.CompilerParams(
            collective_id=1, has_side_effects=True, vmem_limit_bytes=67043328
        ),
        cost_estimate=pl.CostEstimate(
            flops=60 * 10**9, bytes_accessed=32 * rows * half, transcendentals=0
        ),
        name="finish",
    )(shared, weight, grads, partial)


def row_kernel(mine, total, seen, send_sem, recv_sem):
    at = Place()
    groups = seen.shape[0]
    peers = [(k, y) for k in range(2) for y in range(2)]
    barrier = pltpu.get_barrier_semaphore()

    def others(fn):
        for k, y in peers:
            @pl.when(at.group(k, y) != at.c)
            def _():
                fn(k, y)

    others(
        lambda k, y: pl.semaphore_signal(barrier, inc=1, device_id=(at.e, k, y), device_id_type=MESH)
    )
    pl.semaphore_wait(barrier, groups - 1)

    def copy(k, y, slot):
        g = at.group(k, y)
        return send(mine, seen.at[slot], send_sem.at[g], recv_sem.at[slot], (at.e, k, y))

    others(lambda k, y: copy(k, y, at.c).start())
    seen[at.c] = mine[...]
    others(lambda k, y: copy(k, y, at.group(k, y)).wait_recv())
    result = seen[0]
    for g in range(1, groups):
        result = result + seen[g]
    total[...] = result
    others(lambda k, y: copy(k, y, at.c).wait_send())


def sum_rows(rows, groups):
    vmem = pl.BlockSpec(memory_space=pltpu.VMEM)
    return pl.pallas_call(
        row_kernel,
        out_shape=jax.ShapeDtypeStruct(rows.shape, F32),
        in_specs=[vmem],
        out_specs=vmem,
        scratch_shapes=[
            pltpu.VMEM((groups, *rows.shape), F32),
            pltpu.SemaphoreType.DMA((groups,)),
            pltpu.SemaphoreType.DMA((groups,)),
        ],
        compiler_params=pltpu.CompilerParams(collective_id=2, has_side_effects=True),
        name="sum_rows",
    )(rows)


def both_kernel(mine, mine_cols, total, total_cols, seen, seen_cols, r_s, r_r, c_s, c_r):
    at = Place()
    groups, senders = seen.shape[0], seen_cols.shape[0]
    peers = [(k, y) for k in range(2) for y in range(2)]
    barrier = pltpu.get_barrier_semaphore()

    def others(fn):
        for k, y in peers:
            @pl.when(at.group(k, y) != at.c)
            def _():
                fn(k, y)

    def along(fn):
        lax.fori_loop(1, senders, lambda i, carry: (fn(at.other(i)), carry)[1], 0)

    def signal(device):
        pl.semaphore_signal(barrier, inc=1, device_id=device, device_id_type=MESH)

    others(lambda k, y: signal((at.e, k, y)))
    along(lambda d: signal((d, at.k, at.y)))
    pl.semaphore_wait(barrier, groups + senders - 2)

    def copy(k, y, slot):
        g = at.group(k, y)
        return send(mine, seen.at[slot], r_s.at[g], r_r.at[slot], (at.e, k, y))

    def col(d, slot):
        return send(mine_cols, seen_cols.at[slot], c_s.at[d], c_r.at[slot], (d, at.k, at.y))

    others(lambda k, y: copy(k, y, at.c).start())
    along(lambda d: col(d, at.e).start())
    seen[at.c] = mine[...]
    seen_cols[at.e] = mine_cols[...]
    others(lambda k, y: copy(k, y, at.group(k, y)).wait_recv())
    along(lambda d: col(d, d).wait_recv())
    result = seen[0]
    for g in range(1, groups):
        result = result + seen[g]
    total[...] = result
    result = seen_cols[0]
    for d in range(1, senders):
        result = result + seen_cols[d]
    total_cols[...] = result
    others(lambda k, y: copy(k, y, at.c).wait_send())
    along(lambda d: col(d, at.e).wait_send())


def sum_both(rows, cols, groups, senders):
    vmem = pl.BlockSpec(memory_space=pltpu.VMEM)
    dma = pltpu.SemaphoreType.DMA
    return pl.pallas_call(
        both_kernel,
        out_shape=(
            jax.ShapeDtypeStruct(rows.shape, F32),
            jax.ShapeDtypeStruct(cols.shape, F32),
        ),
        in_specs=[vmem, vmem],
        out_specs=(vmem, vmem),
        scratch_shapes=[
            pltpu.VMEM((groups, *rows.shape), F32),
            pltpu.VMEM((senders, *cols.shape), F32),
            dma((groups,)), dma((groups,)), dma((senders,)), dma((senders,)),
        ],
        compiler_params=pltpu.CompilerParams(collective_id=3, has_side_effects=True),
        name="sum_both",
    )(rows, cols)


def owner_body(patches, gain, shift, proj_weight, llm_rank, embed_grad):
    features = ("section", "llmdp")
    own_rows, owned_width = patches.shape
    width = gain.shape[0]
    senders = lax.axis_size("enc")
    most_slots = embed_grad.shape[0] // senders
    groups = width // owned_width
    column_start = lax.axis_index(features) * owned_width
    gain_own = lax.dynamic_slice_in_dim(gain, column_start, owned_width, 0)
    shift_own = lax.dynamic_slice_in_dim(shift, column_start, owned_width, 0)
    values = patches.astype(F32)
    total, squares = sum_rows(jnp.stack([jnp.sum(values, 1), jnp.sum(values * values, 1)]), groups)
    average = (total / width)[:, None]
    variance = (squares / width)[:, None] - average * average
    deviation = lax.rsqrt(variance + EPSILON)
    standardized = (values - average) * deviation
    normed = (standardized * gain_own + shift_own).astype(BF16)

    slot = slots_of(llm_rank, senders, most_slots)
    places = jnp.arange(senders * most_slots, dtype=jnp.int32)
    chosen = (places[:, None] == slot[None, :]).astype(BF16)
    outgoing = jnp.dot(chosen, normed, preferred_element_type=F32).astype(BF16)
    grad_partial, shared, grads, weight = spread(
        outgoing.reshape(senders, most_slots, owned_width), embed_grad, proj_weight
    )
    embeds_recv, returned, grad_sum = finish(
        shared, weight, grads,
        grad_partial.reshape(senders // 2, 2, weight.shape[1], weight.shape[2]),
    )
    grad_weight = grad_sum.astype(F32)
    dnormed = lax.dot_general(
        chosen, returned.reshape(senders * most_slots, owned_width), (((0,), (0,)), ((), ())),
        preferred_element_type=F32,
    )
    dxhat = dnormed * gain_own
    (mean_sum, cross_sum), (gain_gradient, grad_shift) = sum_both(
        jnp.stack([jnp.sum(dxhat, 1), jnp.sum(dxhat * standardized, 1)]),
        jnp.stack([jnp.sum(dnormed * standardized, 0), jnp.sum(dnormed, 0)]),
        groups,
        senders,
    )
    hidden_state_gradient = (
        deviation
        * (dxhat - (mean_sum / width)[:, None] - standardized * (cross_sum / width)[:, None])
    ).astype(BF16)
    return (embeds_recv, hidden_state_gradient, grad_weight, gain_gradient, grad_shift)


def plain_body(patches, gain, shift, proj_weight, llm_rank, embed_grad):
    features = ("section", "llmdp")
    own_rows, owned_width = patches.shape
    width = gain.shape[0]
    weight_rows, out_cols = proj_weight.shape
    senders = lax.axis_size("enc")
    block = block_size(senders, out_cols)
    near = [[b * block + i for i in range(block)] for b in range(senders // block)]
    far = [[b * block + i for b in range(senders // block)] for i in range(block)]

    def near_exchange(x, split, concat):
        return lax.all_to_all(x, "enc", split, concat, axis_index_groups=near, tiled=True)

    column_start = lax.axis_index(features) * owned_width
    gain_own = lax.dynamic_slice_in_dim(gain, column_start, owned_width, 0)

    weight_part = near_exchange(proj_weight, 1, 0)
    weight = lax.all_gather(weight_part, "enc", axis=0, axis_index_groups=far, tiled=True)

    block_rows = lax.all_gather(patches, "enc", axis=0, axis_index_groups=near, tiled=True)
    complete_rows = lax.all_gather(block_rows, features, axis=1, tiled=True).astype(jnp.float32)
    row_average = jnp.mean(complete_rows, 1, keepdims=True)
    variance = jnp.mean(complete_rows * complete_rows, 1, keepdims=True) - row_average * row_average
    inverse_deviation = lax.rsqrt(variance + EPSILON)
    standardized = (complete_rows - row_average) * inverse_deviation
    normed = (standardized * gain + shift).astype(jnp.bfloat16)

    row_start = (lax.axis_index("enc") % block) * own_rows
    average_own = lax.dynamic_slice_in_dim(row_average, row_start, own_rows, 0)
    deviation_own = lax.dynamic_slice_in_dim(inverse_deviation, row_start, own_rows, 0)
    standardized_owned = (patches.astype(jnp.float32) - average_own) * deviation_own

    most_slots = embed_grad.shape[0] // senders
    target = llm_rank[:, 0]
    owners = jnp.arange(senders, dtype=jnp.int32)
    hits = (target[:, None] == owners[None, :]).astype(jnp.int32)
    rank = jnp.sum((jnp.cumsum(hits, 0) - hits) * hits, 1)
    slot = target * most_slots + rank

    def enc_exchange(x):
        return lax.all_to_all(
            x.reshape(senders, most_slots, out_cols), "enc", split_axis=0, concat_axis=0, tiled=True
        ).reshape(senders * most_slots, out_cols)

    d_embed = near_exchange(enc_exchange(embed_grad)[slot], 1, 0)
    grad_part = lax.psum_scatter(
        lax.dot_general(
            normed, d_embed, (((0,), (0,)), ((), ())), preferred_element_type=jnp.float32
        ).astype(jnp.bfloat16),
        "enc",
        scatter_dimension=0,
        axis_index_groups=far,
        tiled=True,
    )
    grad_weight = near_exchange(grad_part, 0, 1).astype(jnp.float32)

    embed_part = jnp.dot(normed, weight, preferred_element_type=jnp.float32).astype(jnp.bfloat16)
    embed = near_exchange(embed_part, 0, 1)
    outgoing = jnp.zeros((senders * most_slots, out_cols), jnp.bfloat16).at[slot].set(embed)
    embeds_recv = enc_exchange(outgoing)

    partial_grad = lax.dot_general(
        d_embed, weight, (((1,), (1,)), ((), ())), preferred_element_type=jnp.float32
    )
    group_count = width // owned_width
    pieces = partial_grad.astype(jnp.bfloat16).reshape(block * own_rows, group_count, owned_width)
    columns = lax.all_to_all(pieces, features, split_axis=1, concat_axis=1, tiled=True)
    column_sum = jnp.sum(columns.astype(jnp.float32), 1).astype(jnp.bfloat16)
    shares = near_exchange(column_sum.reshape(block, own_rows, owned_width), 0, 0)
    owned_normalized_gradient = jnp.sum(shares.astype(jnp.float32), 0)
    owned_centered_gradient = owned_normalized_gradient * gain_own
    mean_sum, cross_sum = lax.psum(
        (
            jnp.sum(owned_centered_gradient, 1),
            jnp.sum(owned_centered_gradient * standardized_owned, 1),
        ),
        features,
    )
    gradient_row_average = (mean_sum / width)[:, None]
    gradient_cross_product = (cross_sum / width)[:, None]
    hidden_state_gradient = (
        deviation_own
        * (
            owned_centered_gradient
            - gradient_row_average
            - standardized_owned * gradient_cross_product
        )
    ).astype(jnp.bfloat16)
    gain_gradient, grad_shift = lax.psum(
        (
            jnp.sum(owned_normalized_gradient * standardized_owned, 0),
            jnp.sum(owned_normalized_gradient, 0),
        ),
        "enc",
    )
    return (embeds_recv, hidden_state_gradient, grad_weight, gain_gradient, grad_shift)


def fits(patches, gain, proj_weight, embed_grad):
    senders, cores, rows_of = (lax.axis_size(a) for a in ("enc", "section", "llmdp"))
    most = embed_grad.shape[0] // senders
    return (
        cores == 2
        and rows_of == 2
        and block_size(senders, proj_weight.shape[1]) == 2
        and senders // 2 == cores * rows_of
        and most % SUBLANES == 0
        and proj_weight.shape[0] % SUBLANES == 0
        and patches.shape[1] == 2 * proj_weight.shape[0]
    )


def body(patches, gain, shift, proj_weight, llm_rank, embed_grad):
    form = owner_body if fits(patches, gain, proj_weight, embed_grad) else plain_body
    return form(patches, gain, shift, proj_weight, llm_rank, embed_grad)


def solution(mesh):
    in_specs = (
        P("enc", ("section", "llmdp")),
        P(),
        P(),
        P("enc", ("section", "llmdp")),
        P("enc", None),
        P("enc", ("section", "llmdp")),
    )
    out_specs = (
        P("enc", ("section", "llmdp")),
        P("enc", ("section", "llmdp")),
        P("enc", ("section", "llmdp")),
        P(("section", "llmdp")),
        P(("section", "llmdp")),
    )
    return jax.shard_map(body, mesh=mesh, in_specs=in_specs, out_specs=out_specs, check_vma=False)
```
